128 devices in a mesh: band: 32 (over z, x, core), sub: 4 (over y).
Axes of the slice: x: 4, y: 4, z: 4, core: 2. Of those that a mesh axis runs over, the one named last changes fastest.
Arguments:
- grad_pred: bfloat16 [227, 98304], P(None, ('band', 'sub')), may hold values from -6 to 6
- grid_latent: bfloat16 [98304, 512], P(('band', 'sub')), may hold values from -6 to 6
- mesh_latent: bfloat16 [40960, 512], P(('band', 'sub')), may hold values from -6 to 6
- send_slot: int32 [98304], P(('band', 'sub')), may hold values from 0 to 2303, as said below
- edge_src: int32 [3, 294912], P(None, ('band', 'sub')), may hold values from 0 to 40959, as said below
- w_mesh: bfloat16 [512, 512], replicated, may hold values from -0.25 to 0.25
- w_grid: bfloat16 [512, 512], replicated, may hold values from -0.25 to 0.25
- w_msg: bfloat16 [512, 512], replicated, may hold values from -0.25 to 0.25
- w_out: bfloat16 [512, 227], replicated, may hold values from -0.25 to 0.25
Outputs:
- mesh_grad: bfloat16 [40960, 512], P(('band', 'sub'))
- grad_w_mesh: float32 [512, 512], replicated
- grad_w_grid: float32 [512, 512], replicated
- grad_w_msg: float32 [512, 512], replicated
- grad_w_out: float32 [512, 227], replicated
The draws below stay inside these ranges and needn't reach their ends.
Inputs may be any that keep to these rules, and one draw needn't show every extreme that they name: For grid point p on latitude-major device i, send_slot[p] = j * 18 + r names patch-major device j and a rank r. On one device i the values are distinct, and for each j the ranks used are 0 to the count of i's points sent to j minus 1. Every such count is at most 18, and 18 is reached in every draw. Every grid point thereby gets one patch-major slot; live slots of each source stand at the front of its block of 18. One patch-major device holds at most 1920 live slots, reached on some device in every draw. `edge_src`: A slot on patch-major device j, of band b = j // 4, names senders in patch b only: mesh rows b * 1280 to (b + 1) * 1280 - 1. Entries of empty slots lie in that range too and are not read.
All inputs are finite; a program needn't handle non-finite values.
Results may differ from the reference program's by a relative error of at most 0.0076.
Values may be sent and summed in bfloat16 or wider, within the bound.
A program may use at most 128 MiB of HBM per device.

```python
import math
import jax
import jax.numpy as jnp

D = 512
C = 227
G_DEV = 768
GRID = 98304
MESH = 40960
PATCH = 1280
CAP = 18
SLOT_DEV = 2304
SLOTS = 294912
N_BAND = 32
N_SUB = 4
DEVICES = 128


def relay_table(key):
    base_count = G_DEV // DEVICES
    half_base = base_count // 2
    receivers = jnp.arange(DEVICES, dtype=jnp.int32)
    band_index = receivers // N_SUB
    polar_band = (band_index < N_BAND // 8) | (band_index >= N_BAND - N_BAND // 8)
    receive_load = jnp.where(polar_band, 5 * half_base, half_base).astype(jnp.int32)
    draw_key, shuffle_key = jax.random.split(jax.random.fold_in(key, 7))
    increments = jax.random.randint(draw_key, (DEVICES,), 0, half_base + 1)
    increments = increments.at[0].set(half_base).at[DEVICES - 1].set(0)
    offsets = (increments - jnp.roll(increments, 1)).astype(jnp.int32)
    senders = jnp.arange(DEVICES, dtype=jnp.int32)
    counts = receive_load[None, :] + offsets[(receivers[None, :] - senders[:, None]) % DEVICES]
    block_ends = jnp.cumsum(counts, axis=1)
    starts = block_ends - counts
    positions = jnp.arange(G_DEV, dtype=jnp.int32)

    def one_sender(row_ends, row_starts, sub_key):
        target = jnp.sum((row_ends[None, :] <= positions[:, None]).astype(jnp.int32), axis=1)
        slot_rank = positions - row_starts[target]
        shuffle = jax.random.permutation(sub_key, G_DEV)
        return jnp.zeros((G_DEV,), jnp.int32).at[shuffle].set(target * CAP + slot_rank)
    sender_keys = jax.random.split(shuffle_key, DEVICES)
    table = jax.vmap(one_sender)(block_ends, starts, sender_keys)
    return table.reshape(GRID).astype(jnp.int32)


def draw_send_slot(key, part):
    return relay_table(key)


def draw_edge_src(key, part):
    local_node = jax.random.randint(jax.random.fold_in(key, 11), (3, SLOTS), 0, PATCH)
    holders = jnp.arange(SLOTS, dtype=jnp.int32) // SLOT_DEV
    band_index = holders // N_SUB
    return (local_node + band_index[None, :] * PATCH).astype(jnp.int32)


def steps_of(rng, shape, cuts, low, largest):
    def one(dim, blocks):
        steps = jax.random.uniform(jax.random.fold_in(jax.random.fold_in(rng, 6), dim), (blocks,), jnp.float32, low / len(cuts), largest / len(cuts))
        return jnp.repeat(jnp.exp(steps), shape[dim] // blocks).reshape((-1,) + (1,) * (len(shape) - dim - 1))

    loudness = one(*cuts[0])
    for cut in cuts[1:]:
        loudness = loudness * one(*cut)
    return loudness


def bell_draw(rng, dims, scale, bound, cuts=(), kind=jnp.bfloat16):
    factor_of = steps_of(rng, dims, cuts, -0.22, 0.18) if cuts else 1.0
    values = jax.random.normal(rng, dims, jnp.float32) * scale * factor_of
    return jnp.minimum(jnp.maximum(values, -bound), bound).astype(kind)


def setup_inputs(seed: int = 0) -> dict:
    seeds = jax.random.split(jax.random.key(seed), 10)
    grad_pred = bell_draw(seeds[0], (C, GRID), 1.0, 6.0, ((1, 128),))
    grid_latent = bell_draw(seeds[1], (GRID, D), 1.0, 6.0, ((0, 128),))
    mesh_latent = bell_draw(seeds[2], (MESH, D), 1.0, 6.0, ((0, 128),))
    send_slot = draw_send_slot(jax.random.fold_in(seeds[9], 71), 0)
    edge_src = draw_edge_src(jax.random.fold_in(seeds[9], 71), 0)
    w_mesh = bell_draw(seeds[5], (D, D), D ** -0.5, 0.25)
    w_grid = bell_draw(seeds[6], (D, D), D ** -0.5, 0.25)
    w_msg = bell_draw(seeds[7], (D, D), D ** -0.5, 0.25)
    w_out = bell_draw(seeds[8], (D, C), D ** -0.5, 0.25)
    return {"grad_pred": grad_pred, "grid_latent": grid_latent, "mesh_latent": mesh_latent, "send_slot": send_slot, "edge_src": edge_src, "w_mesh": w_mesh, "w_grid": w_grid, "w_msg": w_msg, "w_out": w_out}


def latitude_weight(points, total):
    angle = jnp.pi * ((points.astype(jnp.float32) + 0.5) / total - 0.5)
    return 0.5 * jnp.pi * jnp.cos(angle)

def silu_slope(value):
    sigma = jax.nn.sigmoid(value)
    return sigma * (1.0 + value * (1.0 - sigma))

def reference(grad_pred, grid_latent, mesh_latent, send_slot, edge_src, w_mesh, w_grid, w_msg, w_out):
    points = jnp.arange(GRID, dtype=jnp.int32)
    source_dev = (points // G_DEV).astype(jnp.int32)
    target = (send_slot // CAP).astype(jnp.int32)
    slot_rank = (send_slot % CAP).astype(jnp.int32)
    holder = (target * SLOT_DEV + source_dev * CAP + slot_rank).astype(jnp.int32)
    senders = edge_src[:, holder]
    grid_proj = jnp.dot(grid_latent, w_grid, preferred_element_type=jnp.float32).astype(jnp.bfloat16)
    mesh_proj = jnp.dot(mesh_latent, w_mesh, preferred_element_type=jnp.float32).astype(jnp.bfloat16)
    grid_float = grid_proj.astype(jnp.float32)
    pre_acts = [mesh_proj[senders[corner]].astype(jnp.float32) + grid_float for corner in range(3)]
    act_sum = (jax.nn.silu(pre_acts[0]) + jax.nn.silu(pre_acts[1]) + jax.nn.silu(pre_acts[2])).astype(jnp.bfloat16)
    aggregate = jnp.dot(act_sum, w_msg, preferred_element_type=jnp.float32).astype(jnp.bfloat16)
    weighted = (latitude_weight(points, GRID)[None, :] * grad_pred.astype(jnp.float32)).astype(jnp.bfloat16)
    raw_out = jnp.dot(aggregate.T, weighted.T, preferred_element_type=jnp.float32)
    agg_grad = jnp.dot(weighted.T, w_out.T, preferred_element_type=jnp.float32).astype(jnp.bfloat16)
    raw_msg = jnp.dot(act_sum.T, agg_grad, preferred_element_type=jnp.float32)
    act_grad = jnp.dot(agg_grad, w_msg.T, preferred_element_type=jnp.float32)
    pre_grads = [(act_grad * silu_slope(pre)).astype(jnp.bfloat16) for pre in pre_acts]
    grid_proj_grad = (pre_grads[0].astype(jnp.float32) + pre_grads[1].astype(jnp.float32) + pre_grads[2].astype(jnp.float32)).astype(jnp.bfloat16)
    raw_grid = jnp.dot(grid_latent.T, grid_proj_grad, preferred_element_type=jnp.float32)
    node_total = jnp.zeros((MESH, D), jnp.float32)
    for corner in range(3):
        node_total = node_total.at[senders[corner]].add(pre_grads[corner].astype(jnp.float32))
    mesh_proj_grad = node_total.astype(jnp.bfloat16)
    mesh_grad = jnp.dot(mesh_proj_grad, w_mesh.T, preferred_element_type=jnp.float32).astype(jnp.bfloat16)
    raw_mesh = jnp.dot(mesh_latent.T, mesh_proj_grad, preferred_element_type=jnp.float32)
    grad_scale = 1.0 / math.sqrt(3.0 * GRID)
    return (mesh_grad, raw_mesh * grad_scale, raw_grid * grad_scale, raw_msg * grad_scale, raw_out * grad_scale)
```

```python
import functools
import math

import jax
import jax.numpy as jnp
from jax import lax
from jax.experimental import pallas as pl
from jax.experimental.pallas import tpu as pltpu
from jax.sharding import PartitionSpec as P

MESH = pl.DeviceIdType.MESH
BF, F32 = jnp.bfloat16, jnp.float32
MAIN, OVER = 16, 2
CAP = MAIN + OVER
NDEV = 128
NN = (((1,), (0,)), ((), ()))
NT = (((1,), (1,)), ((), ()))
TN = (((0,), (0,)), ((), ()))
STRIDE, INVERSE = 37, 45


def dot(a, b, dims):
    return lax.dot_general(a, b, dims, preferred_element_type=F32)


def place():
    band, sub = lax.axis_index("band"), lax.axis_index("sub")
    return band // 8, (band // 2) % 4, band % 2, sub


def offset(d):
    e = (d * STRIDE) % NDEV
    return (e // 16) % 4, (e // 4) % 4, e // 64, e % 4


def peer(d):
    z, x, c, y = place()
    dz, dx, dc, dy = offset(d)
    return ((z + dz) % 4) * 8 + ((x + dx) % 4) * 2 + (c + dc) % 2, (y + dy) % 4


def source(d):
    z, x, c, y = place()
    dz, dx, dc, dy = offset(d)
    band = ((z - dz + 4) % 4) * 8 + ((x - dx + 4) % 4) * 2 + (c + dc) % 2
    return band * 4 + (y - dy + 4) % 4


ROWS = 256
GROUPS = NDEV * CAP // ROWS
BLOCKS = ROWS // MAIN
CHIPS = 64


def chip_peer(q):
    z, x, c, y = place()
    p = (q * 37) % CHIPS
    z, x, y = (z + p // 16) % 4, (x + (p // 4) % 4) % 4, (y + p % 4) % 4
    return (z * 8 + x * 2 + c, y), (z * 4 + x) * 4 + y


def remote(src, dst, send, recv, device):
    return pltpu.make_async_remote_copy(
        src_ref=src,
        dst_ref=dst,
        send_sem=send,
        recv_sem=recv,
        device_id=device,
        device_id_type=MESH,
    )


def kernel(
    grad_ref,
    latent_ref,
    mesh_ref,
    slot_ref,
    index_ref,
    w_mesh_ref,
    w_grid_ref,
    w_msg_ref,
    w_out_ref,
    sums_ref,
    proj_ref,
    weighted,
    main_send,
    over_send,
    main_recv,
    over_recv,
    patch,
    table,
    back,
    node,
    node_send,
    node_recv,
    rows_ref,
    pre_grad,
    part,
    pair_recv,
    rs_send,
    rs_recv,
    ag_send,
    main_ssem,
    main_rsem,
    ssem,
    rsem,
):
    z, x, c, y = place()
    band = lax.axis_index("band")
    sibling = (band + 1 - 2 * c, y)
    bar = pltpu.get_barrier_semaphore()

    def greet(d, carry):
        pl.semaphore_signal(bar, inc=1, device_id=peer(d), device_id_type=MESH)
        return carry

    lax.fori_loop(1, NDEV, greet, 0)

    channels, points = grad_ref.shape
    me = band * 4 + y
    lane = lax.broadcasted_iota(jnp.int32, (1, points), 1)
    total = points * NDEV
    angle = jnp.pi * (((me * points + lane).astype(F32) + 0.5) / total - 0.5)
    weight = 0.5 * jnp.pi * jnp.cos(angle)
    weighted[...] = jnp.zeros_like(weighted)
    weighted[0:channels, :] = (weight * grad_ref[...].astype(F32)).astype(BF)
    slot = slot_ref[...]
    j = (slot * 3641) >> 16
    r = slot - j * CAP
    e = (
        ((j - y) & 3)
        + 4 * (((j >> 3) - x) & 3)
        + 16 * (((j >> 5) - z) & 3)
        + 64 * (((j >> 2) - c) & 1)
    )
    d = (e * INVERSE) & (NDEV - 1)
    at_main = jnp.where(r < MAIN, d * MAIN + r, -1)
    at_over = jnp.where(r >= MAIN, d * OVER + r - MAIN, -1)
    row = lax.broadcasted_iota(jnp.int32, (ROWS, points), 0)

    def pick(at, base):
        hot = jnp.where(row == at - base, 1.0, 0.0).astype(BF)
        lat = dot(hot, latent_ref[...], NN).astype(BF)
        gr = dot(hot, weighted[...], NT).astype(BF)
        return lat, gr

    lat, gr = pick(at_over, 0)
    over_send[:, :, 0:512] = lat.reshape(NDEV, OVER, 512)
    over_send[:, :, 512:768] = gr.reshape(NDEV, OVER, 256)
    over_recv[0] = over_send[0]
    patch[y] = mesh_ref[...]

    def pick_main(g):
        lat, gr = pick(at_main, g * ROWS)
        blocks = pl.ds(g * BLOCKS, BLOCKS)
        main_send[blocks, :, 0:512] = lat.reshape(BLOCKS, MAIN, 512)
        main_send[blocks, :, 512:768] = gr.reshape(BLOCKS, MAIN, 256)

    pick_main(0)
    main_recv[0] = main_send[0]
    pl.semaphore_wait(bar, NDEV - 1)

    def patch_copy(k):
        return remote(
            mesh_ref, patch.at[y], ssem.at[0], rsem.at[0], (band, (y + k) % 4)
        )

    for k in (1, 2, 3):
        patch_copy(k).start()

    def send_over(d, carry):
        remote(
            over_send.at[d], over_recv.at[d], ssem.at[1], rsem.at[1], peer(d)
        ).start()
        return carry

    lax.fori_loop(1, NDEV, send_over, 0)

    def send_main(d, carry):
        remote(
            main_send.at[d], main_recv.at[d], main_ssem.at[0], main_rsem.at[d // BLOCKS], peer(d)
        ).start()
        return carry

    lax.fori_loop(1, BLOCKS, send_main, 0)

    def prep_group(g, carry):
        pick_main(g)
        lax.fori_loop(g * BLOCKS, (g + 1) * BLOCKS, send_main, 0)
        return carry

    lax.fori_loop(1, GROUPS - 1, prep_group, 0)

    back[...] = jnp.zeros_like(back)
    back[:, 0:channels] = dot(w_msg_ref[...], w_out_ref[...], NN).astype(BF)
    node[...] = jnp.zeros_like(node)
    part[...] = jnp.zeros_like(part)
    remote(
        patch.at[pl.ds(0, 3)], patch.at[pl.ds(0, 3)], ssem.at[0], rsem.at[0], sibling
    ).wait_recv()
    for k in range(4):
        table[pl.ds(k * 320, 320), :] = dot(patch[k], w_mesh_ref[...], NN).astype(BF)
    size = table.shape[0]

    def group(g):
        latent, grad = rows_ref[:, 0:512], rows_ref[:, 512:768]
        grid_proj = dot(latent, w_grid_ref[...], NN).astype(BF).astype(F32)
        act_grad = dot(grad, back[...], NT)
        index = index_ref[g]
        column = index.T
        node_col = lax.broadcasted_iota(jnp.int32, (ROWS, size), 1)
        node_row = lax.broadcasted_iota(jnp.int32, (size, ROWS), 0)
        act = jnp.zeros((ROWS, 512), F32)
        total = jnp.zeros((ROWS, 512), F32)
        for k in range(3):
            hot = jnp.where(node_col == column[:, k : k + 1], 1.0, 0.0).astype(BF)
            pre = dot(hot, table[...], NN) + grid_proj
            sigma = 0.5 * jnp.tanh(0.5 * pre) + 0.5
            value = pre * sigma
            act += value
            grad_k = (act_grad * (sigma + value * (1.0 - sigma))).astype(BF)
            total += grad_k.astype(F32)
            pre_grad[pl.ds(k * ROWS, ROWS), :] = grad_k
        act = act.astype(BF)
        moment = dot(act, grad, TN)
        part[0, :, 512:640] += moment[:, 0:128]
        part[1, :, 512:640] += moment[:, 128:256]
        part[1, :, 0:512] += dot(latent, total.astype(BF), TN)
        hots = [
            jnp.where(node_row == index[k : k + 1, :], 1.0, 0.0).astype(BF)
            for k in range(3)
        ]
        node[...] += dot(jnp.concatenate(hots, axis=1), pre_grad[...], NN)

    def await_main(g, first, count):
        blocks = pl.ds(first, count)
        remote(
            main_send.at[blocks], main_recv.at[blocks], main_ssem.at[0], main_rsem.at[g], sibling
        ).wait_recv()

    def step(g, carry):
        @pl.when(g == 0)
        def _():
            blocks = pl.ds(1, NDEV - 1)
            remote(
                over_send.at[blocks], over_recv.at[blocks], ssem.at[1], rsem.at[1], sibling
            ).wait_recv()
            rows_ref[...] = over_recv[...].reshape(ROWS, 768)

        @pl.when(g == 1)
        def _():
            await_main(0, 1, BLOCKS - 1)

        @pl.when(g > 1)
        def _():
            await_main(g - 1, (g - 1) * BLOCKS, BLOCKS)

        @pl.when(g > 0)
        def _():
            blocks = pl.ds((g - 1) * BLOCKS, BLOCKS)
            rows_ref[...] = main_recv[blocks, :, :].reshape(ROWS, 768)

        group(g)
        return carry

    lax.fori_loop(0, GROUPS, step, 0)

    def node_copy(k):
        to = (y + k) % 4
        return remote(
            node_send.at[to], node_recv.at[k - 1], ssem.at[2], rsem.at[2], (band, to)
        )

    for k in range(4):
        node_send[k] = node[pl.ds(k * 320, 320), :].astype(BF)
    mesh_part = dot(patch[0], node_send[0], TN)
    for k in (1, 2, 3):
        mesh_part += dot(patch[k], node_send[k], TN)
    part[0, :, 0:512] = mesh_part
    pair = remote(part.at[1 - c], pair_recv, ssem.at[3], rsem.at[3], sibling)
    pair.start()
    for k in (1, 2, 3):
        node_copy(k).start()
    pair.wait_recv()
    rs_send[...] = (part[c] + pair_recv[...]).astype(BF).reshape(CHIPS, 8, 640)

    def scatter(q, carry):
        device, chip = chip_peer(q)
        remote(rs_send.at[chip], rs_recv.at[q], ssem.at[4], rsem.at[4], device).start()
        return carry

    lax.fori_loop(1, CHIPS, scatter, 0)
    own, chip = chip_peer(0)
    rs_recv[0] = rs_send[chip]

    remote(
        node_send.at[pl.ds(0, 3)], node_recv, ssem.at[2], rsem.at[2], sibling
    ).wait_recv()
    mine = node[pl.ds(y * 320, 320), :]
    proj_ref[...] = (
        mine + node_recv[0].astype(F32) + node_recv[1].astype(F32) + node_recv[2].astype(F32)
    ).astype(BF)

    others = pl.ds(1, CHIPS - 1)
    remote(
        rs_send.at[others], rs_recv.at[others], ssem.at[4], rsem.at[4], sibling
    ).wait_recv()
    scale = 1.0 / math.sqrt(3.0 * points * NDEV)
    ag_send[...] = (jnp.sum(rs_recv[...].astype(F32), axis=0) * scale).astype(BF)
    sums_ref[c, chip] = ag_send[...]

    def gather(q, carry):
        device, _ = chip_peer(q)
        remote(ag_send, sums_ref.at[c, chip], ssem.at[5], rsem.at[5], device).start()
        return carry

    lax.fori_loop(1, CHIPS, gather, 0)
    most = sums_ref.at[c, pl.ds(0, CHIPS - 1)]
    remote(most, most, ssem.at[5], rsem.at[5], sibling).wait_recv()
    share = remote(sums_ref.at[c], sums_ref.at[c], ssem.at[6], rsem.at[6], sibling)
    share.start()

    three = node_send.at[pl.ds(0, 3)]
    remote(patch.at[pl.ds(0, 3)], patch.at[pl.ds(0, 3)], ssem.at[0], rsem.at[0], sibling).wait_send()
    blocks = pl.ds(1, NDEV - 1)
    remote(over_send.at[blocks], over_recv.at[blocks], ssem.at[1], rsem.at[1], sibling).wait_send()
    remote(main_send.at[blocks], main_recv.at[blocks], main_ssem.at[0], main_rsem.at[0], sibling).wait_send()
    remote(three, node_recv, ssem.at[2], rsem.at[2], sibling).wait_send()
    pair.wait_send()
    remote(rs_send.at[others], rs_recv.at[others], ssem.at[4], rsem.at[4], sibling).wait_send()
    remote(most, most, ssem.at[5], rsem.at[5], sibling).wait_send()
    share.wait()


def final_kernel(sums_ref, proj_ref, w_mesh_ref, w_msg_ref, w_out_ref, node_ref, mesh_ref, grid_ref, msg_ref, out_ref):
    node_ref[...] = dot(proj_ref[...], w_mesh_ref[...], NT).astype(BF)
    mesh_ref[...] = sums_ref[0, :, :, 0:512].astype(F32).reshape(512, 512)
    grid_ref[...] = sums_ref[1, :, :, 0:512].astype(F32).reshape(512, 512)
    low = sums_ref[0, :, :, 512:640].astype(F32).reshape(512, 128)
    high = sums_ref[1, :, :, 512:640].astype(F32).reshape(512, 128)
    moment = jnp.concatenate([low, high], axis=1)[:, 0:227].astype(BF)
    msg_ref[...] = dot(moment, w_out_ref[...], NT)
    out_ref[...] = dot(w_msg_ref[...], moment, TN)


def shards(grad_pred, grid_latent, mesh_latent, send_slot, edge_src, w_mesh, w_grid, w_msg, w_out):
    band = lax.axis_index("band")
    order = source(jnp.arange(NDEV, dtype=jnp.int32))
    local = (edge_src - band * 1280).reshape(3, NDEV, CAP)[:, order, :]
    head = local[:, :, :MAIN].reshape(3, GROUPS - 1, ROWS).transpose(1, 0, 2)
    tail = local[:, :, MAIN:].reshape(3, 1, ROWS).transpose(1, 0, 2)
    index = jnp.concatenate([tail, head], axis=0)
    index = jnp.pad(index, ((0, 0), (0, 5), (0, 0)))
    vmem = pltpu.VMEM
    sums, proj = pl.pallas_call(
        kernel,
        out_shape=[
            jax.ShapeDtypeStruct((2, CHIPS, 8, 640), BF),
            jax.ShapeDtypeStruct((320, 512), BF),
        ],
        scratch_shapes=[
            vmem((256, 768), BF),
            vmem((NDEV, MAIN, 768), BF),
            vmem((NDEV, OVER, 768), BF),
            vmem((NDEV, MAIN, 768), BF),
            vmem((NDEV, OVER, 768), BF),
            vmem((4, 320, 512), BF),
            vmem((1280, 512), BF),
            vmem((512, 256), BF),
            vmem((1280, 512), F32),
            vmem((4, 320, 512), BF),
            vmem((3, 320, 512), BF),
            vmem((ROWS, 768), BF),
            vmem((3 * ROWS, 512), BF),
            vmem((2, 512, 640), F32),
            vmem((512, 640), F32),
            vmem((CHIPS, 8, 640), BF),
            vmem((CHIPS, 8, 640), BF),
            vmem((8, 640), BF),
            pltpu.SemaphoreType.DMA((1,)),
            pltpu.SemaphoreType.DMA((GROUPS - 1,)),
            pltpu.SemaphoreType.DMA((7,)),
            pltpu.SemaphoreType.DMA((7,)),
        ],
        compiler_params=pltpu.CompilerParams(
            collective_id=0, has_side_effects=True, vmem_limit_bytes=63 * 2**20
        ),
    )(
        grad_pred,
        grid_latent,
        mesh_latent,
        send_slot.reshape(1, -1),
        index,
        w_mesh,
        w_grid,
        w_msg,
        w_out,
    )
    return pl.pallas_call(
        final_kernel,
        out_shape=[
            jax.ShapeDtypeStruct((320, 512), BF),
            jax.ShapeDtypeStruct((512, 512), F32),
            jax.ShapeDtypeStruct((512, 512), F32),
            jax.ShapeDtypeStruct((512, 512), F32),
            jax.ShapeDtypeStruct((512, 227), F32),
        ],
        compiler_params=pltpu.CompilerParams(vmem_limit_bytes=40 * 2**20),
    )(sums, proj, w_mesh, w_msg, w_out)


def solution(mesh):
    both = ("band", "sub")
    placed = (P(None, both), P(both, None), P(both, None), P(both), P(None, both))
    return jax.shard_map(
        shards,
        mesh=mesh,
        in_specs=placed + (P(),) * 4,
        out_specs=(P(both, None), P(), P(), P(), P()),
        check_vma=False,
    )
```

```python
import functools
import math

import jax
import jax.numpy as jnp
from jax import lax
from jax.experimental import pallas as pl
from jax.experimental.pallas import tpu as pltpu
from jax.sharding import PartitionSpec as P

MESH = pl.DeviceIdType.MESH
BF, F32 = jnp.bfloat16, jnp.float32
MAIN, OVER = 16, 2
CAP = MAIN + OVER
NDEV = 128
NN = (((1,), (0,)), ((), ()))
NT = (((1,), (1,)), ((), ()))
TN = (((0,), (0,)), ((), ()))
MIX, UNMIX = 13, 5


def dot(a, b, dims):
    return lax.dot_general(a, b, dims, preferred_element_type=F32)


def place():
    band, sub = lax.axis_index("band"), lax.axis_index("sub")
    return lax.div(band, 8), lax.rem(lax.div(band, 2), 4), lax.rem(band, 2), sub


def shifted(u, dy):
    z, x, c, y = place()
    z = lax.rem(z + lax.rem(u, 4), 4)
    x = lax.rem(x + lax.rem(lax.div(u, 4), 4), 4)
    c = lax.rem(c + lax.div(u, 16), 2)
    return z * 8 + x * 2 + c, lax.rem(y + dy, 4)


def near(d):
    return shifted(lax.rem(d * MIX, 32), 0)


def far(d):
    t = d - 32
    q = lax.div(t, 3)
    return shifted(lax.rem(q * MIX, 32), 1 + t - 3 * q)


def source(d):
    z, x, c, y = place()
    t = jnp.maximum(d - 32, 0)
    q = (t * 171) >> 9
    u = jnp.where(d < 32, (d * MIX) & 31, (q * MIX) & 31)
    dy = jnp.where(d < 32, 0, 1 + t - 3 * q)
    band = ((z - u) & 3) * 8 + ((x - (u >> 2)) & 3) * 2 + ((c - (u >> 4)) & 1)
    return band * 4 + ((y - dy) & 3)


ROWS = 256
GROUPS = NDEV * CAP // ROWS
BLOCKS = ROWS // MAIN
CHIPS = 64
SLOTS = NDEV * CAP


def chip_peer(q):
    z, x, c, y = place()
    p = lax.rem(q * 37, CHIPS)
    z = lax.rem(z + lax.div(p, 16), 4)
    x = lax.rem(x + lax.rem(lax.div(p, 4), 4), 4)
    return z * 8 + x * 2 + c, lax.rem(y + lax.rem(p, 4), 4)


def plane_peer(q):
    z, x, c, y = place()
    p = lax.rem(q * 5, 16)
    z = lax.rem(z + lax.div(p, 4), 4)
    x = lax.rem(x + lax.rem(p, 4), 4)
    return (z * 8 + x * 2 + c, y), z * 4 + x


def remote(src, dst, send, recv, device):
    return pltpu.make_async_remote_copy(
        src_ref=src,
        dst_ref=dst,
        send_sem=send,
        recv_sem=recv,
        device_id=device,
        device_id_type=MESH,
    )


def kernel(
    grad_in,
    latent_in,
    mesh_in,
    slot_in,
    edge_in,
    w_mesh_in,
    w_grid_in,
    w_msg_in,
    w_out_in,
    sums_ref,
    proj_ref,
    grad_ref,
    latent_ref,
    slot_ref,
    edge_ref,
    w_mesh_ref,
    w_grid_ref,
    w_msg_ref,
    w_out_ref,
    load_sem,
    index_ref,
    gathered,
    weighted,
    main_send,
    over_send,
    main_recv,
    over_recv,
    patch,
    table,
    back,
    node,
    node_send,
    node_recv,
    rows_ref,
    pre_grad,
    part,
    pair_recv,
    rs_send,
    rs_recv,
    ring_send,
    ring_recv,
    ag_send,
    main_ssem,
    main_rsem,
    ssem,
    rsem,
):
    z, x, c, y = place()
    band = lax.axis_index("band")
    sibling = (band + 1 - 2 * c, y)
    loads = [
        pltpu.make_async_copy(src, dst, load_sem.at[k])
        for k, (src, dst) in enumerate(
            (
                (grad_in, grad_ref),
                (slot_in, slot_ref),
                (latent_in, latent_ref),
                (mesh_in, patch.at[y]),
                (edge_in, edge_ref),
                (w_msg_in, w_msg_ref),
                (w_out_in, w_out_ref),
                (w_mesh_in, w_mesh_ref),
                (w_grid_in, w_grid_ref),
            )
        )
    ]
    for load in loads:
        load.start()
    bar = pltpu.get_barrier_semaphore()

    def each(peer, act):
        def run(d, carry):
            act(d, peer(d))
            return carry

        return run

    def greet(d, device):
        pl.semaphore_signal(bar, inc=1, device_id=device, device_id_type=MESH)

    lax.fori_loop(1, 32, each(near, greet), 0)
    lax.fori_loop(32, NDEV, each(far, greet), 0)
    pl.semaphore_wait(bar, NDEV - 1)
    for k in (1, 2, 3):
        remote(
            mesh_in, patch.at[y], ssem.at[0], rsem.at[0], (band, lax.rem(y + k, 4))
        ).start()

    for load in loads:
        load.wait()
    channels, points = grad_ref.shape
    me = band * 4 + y
    lane = lax.broadcasted_iota(jnp.int32, (1, points), 1)
    total = points * NDEV
    angle = jnp.pi * (((me * points + lane).astype(F32) + 0.5) / total - 0.5)
    weight = 0.5 * jnp.pi * jnp.cos(angle)
    weighted[...] = jnp.zeros_like(weighted)
    weighted[0:channels, :] = (weight * grad_ref[...].astype(F32)).astype(BF)
    slot = slot_ref[...].reshape(1, points)
    j = (slot * 3641) >> 16
    r = slot - j * CAP
    dy = (j - y) & 3
    u = (((j >> 5) - z) & 3) + 4 * (((j >> 3) - x) & 3) + 16 * (((j >> 2) - c) & 1)
    q = (u * UNMIX) & 31
    d = jnp.where(dy == 0, q, 31 + 3 * q + dy)
    at_main = jnp.where(r < MAIN, d * MAIN + r, -1)
    at_over = jnp.where(r >= MAIN, d * OVER + r - MAIN, -1)
    row = lax.broadcasted_iota(jnp.int32, (ROWS, points), 0)

    def pick(at, base):
        hot = jnp.where(row == at - base, 1.0, 0.0).astype(BF)
        lat = dot(hot, latent_ref[...], NN).astype(BF)
        gr = dot(hot, weighted[...], NT).astype(BF)
        return lat, gr

    lat, gr = pick(at_over, 0)
    over_send[:, :, 0:512] = lat.reshape(NDEV, OVER, 512)
    over_send[:, :, 512:768] = gr.reshape(NDEV, OVER, 256)
    over_recv[0] = over_send[0]

    def pick_main(g):
        lat, gr = pick(at_main, g * ROWS)
        blocks = pl.ds(g * BLOCKS, BLOCKS)
        main_send[blocks, :, 0:512] = lat.reshape(BLOCKS, MAIN, 512)
        main_send[blocks, :, 512:768] = gr.reshape(BLOCKS, MAIN, 256)

    def send_over(d, device):
        remote(
            over_send.at[d], over_recv.at[d], ssem.at[1], rsem.at[1], device
        ).start()

    def send_main(d, device):
        remote(
            main_send.at[d],
            main_recv.at[d],
            main_ssem.at[0],
            main_rsem.at[lax.div(d, BLOCKS)],
            device,
        ).start()

    pick_main(0)
    pick_main(1)
    main_recv[0] = main_send[0]
    lax.fori_loop(1, 32, each(near, send_main), 0)
    lax.fori_loop(1, 32, each(near, send_over), 0)

    def prep_group(g, carry):
        pick_main(g)
        return carry

    lax.fori_loop(2, GROUPS - 1, prep_group, 0)
    back[...] = jnp.zeros_like(back)
    back[:, 0:channels] = dot(w_msg_ref[...], w_out_ref[...], NT).astype(BF)
    node[...] = jnp.zeros_like(node)
    part[...] = jnp.zeros_like(part)

    size = table.shape[0]
    local = edge_ref[...] - band * size
    halves = jnp.concatenate(
        [(local >> 4).astype(F32), (local & 15).astype(F32), jnp.zeros((2, SLOTS), F32)], axis=0
    ).astype(BF)
    lanes = lax.broadcasted_iota(jnp.int32, (ROWS, SLOTS), 1)
    line = lax.broadcasted_iota(jnp.int32, (ROWS, 1), 0)

    def find(g, slots):
        hot = jnp.where(lanes == slots, 1.0, 0.0).astype(BF)
        found = dot(halves, hot, NT)
        whole = (found[0:3] * 16.0 + found[3:6]).astype(jnp.int32)
        index_ref[g, 0:3, :] = whole

    def find_main(g, carry):
        find(g, source((g - 1) * BLOCKS + (line >> 4)) * CAP + (line & 15))
        return carry

    index_ref[...] = jnp.zeros_like(index_ref)
    find(0, source(line >> 1) * CAP + MAIN + (line & 1))
    lax.fori_loop(1, GROUPS, find_main, 0)

    remote(
        patch.at[pl.ds(0, 3)], patch.at[pl.ds(0, 3)], ssem.at[0], rsem.at[0], sibling
    ).wait_recv()
    lax.fori_loop(32, NDEV, each(far, send_over), 0)
    lax.fori_loop(32, NDEV, each(far, send_main), 0)
    for k in range(4):
        table[pl.ds(k * 320, 320), :] = dot(patch[k], w_mesh_ref[...], NN).astype(BF)

    def collect(g, carry):
        column = index_ref[g].T
        node_col = lax.broadcasted_iota(jnp.int32, (ROWS, size), 1)
        for k in range(3):
            hot = jnp.where(node_col == column[:, k : k + 1], 1.0, 0.0).astype(BF)
            gathered[g, k] = dot(hot, table[...], NN).astype(BF)
        return carry

    lax.fori_loop(0, GROUPS, collect, 0)

    def group(g):
        latent, grad = rows_ref[:, 0:512], rows_ref[:, 512:768]
        grid_proj = dot(latent, w_grid_ref[...], NN).astype(BF).astype(F32)
        act_grad = dot(grad, back[...], NT)
        index = index_ref[g]
        node_row = lax.broadcasted_iota(jnp.int32, (size, ROWS), 0)
        act = jnp.zeros((ROWS, 512), F32)
        total = jnp.zeros((ROWS, 512), F32)
        for k in range(3):
            pre = gathered[g, k].astype(F32) + grid_proj
            sigma = 0.5 * jnp.tanh(0.5 * pre) + 0.5
            value = pre * sigma
            act += value
            grad_k = (act_grad * (sigma + value * (1.0 - sigma))).astype(BF)
            total += grad_k.astype(F32)
            pre_grad[pl.ds(k * ROWS, ROWS), :] = grad_k
        act = act.astype(BF)
        moment = dot(act, grad, TN)
        part[0, :, 512:640] += moment[:, 0:128]
        part[1, :, 512:640] += moment[:, 128:256]
        part[1, :, 0:512] += dot(latent, total.astype(BF), TN)
        hots = [
            jnp.where(node_row == index[k : k + 1, :], 1.0, 0.0).astype(BF)
            for k in range(3)
        ]
        node[...] += dot(jnp.concatenate(hots, axis=1), pre_grad[...], NN)

    def await_main(g, first, count):
        blocks = pl.ds(first, count)
        remote(
            main_send.at[blocks], main_recv.at[blocks], main_ssem.at[0], main_rsem.at[g], sibling
        ).wait_recv()

    def load_main(g):
        blocks = pl.ds(g * BLOCKS, BLOCKS)
        rows_ref[...] = main_recv[blocks, :, :].reshape(ROWS, 768)

    def step(i, carry):
        @pl.when(i == 0)
        def _():
            await_main(0, 1, BLOCKS - 1)
            load_main(0)

        @pl.when(i == 1)
        def _():
            await_main(1, BLOCKS, BLOCKS)
            load_main(1)

        @pl.when(i == 2)
        def _():
            blocks = pl.ds(1, NDEV - 1)
            remote(
                over_send.at[blocks], over_recv.at[blocks], ssem.at[1], rsem.at[1], sibling
            ).wait_recv()
            rows_ref[...] = over_recv[...].reshape(ROWS, 768)

        @pl.when(i > 2)
        def _():
            await_main(i - 1, (i - 1) * BLOCKS, BLOCKS)
            load_main(i - 1)

        group(jnp.where(i < 2, i + 1, jnp.where(i == 2, 0, i)))
        return carry

    lax.fori_loop(0, GROUPS, step, 0)

    def node_copy(k):
        to = (y + k) % 4
        return remote(
            node_send.at[to], node_recv.at[k - 1], ssem.at[2], rsem.at[2], (band, to)
        )

    for k in range(4):
        node_send[k] = node[pl.ds(k * 320, 320), :].astype(BF)
    for k in (1, 2, 3):
        node_copy(k).start()
    mesh_part = dot(patch[0], node_send[0], TN)
    for k in (1, 2, 3):
        mesh_part += dot(patch[k], node_send[k], TN)
    part[0, :, 0:512] = mesh_part
    pair = remote(part.at[1 - c], pair_recv, ssem.at[3], rsem.at[3], sibling)
    pair.start()
    pair.wait_recv()
    rs_send[...] = (part[c] + pair_recv[...]).astype(BF).reshape(16, 32, 640)

    def scatter(q, carry):
        device, plane = plane_peer(q)
        remote(rs_send.at[plane], rs_recv.at[q], ssem.at[4], rsem.at[4], device).start()
        return carry

    lax.fori_loop(1, 16, scatter, 0)
    plane = z * 4 + x
    rs_recv[0] = rs_send[plane]
    others = pl.ds(1, 15)
    scattered = remote(
        rs_send.at[others], rs_recv.at[others], ssem.at[4], rsem.at[4], sibling
    )
    scattered.wait_recv()
    plane_sum = rs_recv[0].astype(F32)
    for k in range(1, 16):
        plane_sum += rs_recv[k].astype(F32)
    ring_send[...] = plane_sum.astype(BF).reshape(4, 8, 640)
    for k in (1, 2, 3):
        to = lax.rem(y + k, 4)
        remote(
            ring_send.at[to], ring_recv.at[k - 1], ssem.at[7], rsem.at[7], (band, to)
        ).start()
    ring = remote(
        ring_send.at[pl.ds(0, 3)], ring_recv, ssem.at[7], rsem.at[7], sibling
    )
    ring.wait_recv()
    full = ring_send[y].astype(F32)
    for k in range(3):
        full += ring_recv[k].astype(F32)
    chip = plane * 4 + y
    scale = 1.0 / math.sqrt(3.0 * points * NDEV)
    ag_send[...] = (full * scale).astype(BF)
    sums_ref[c, chip] = ag_send[...]

    def gather(q, carry):
        remote(
            ag_send, sums_ref.at[c, chip], ssem.at[5], rsem.at[5], chip_peer(q)
        ).start()
        return carry

    lax.fori_loop(1, CHIPS, gather, 0)

    remote(
        node_send.at[pl.ds(0, 3)], node_recv, ssem.at[2], rsem.at[2], sibling
    ).wait_recv()
    mine = node[pl.ds(y * 320, 320), :]
    proj_ref[...] = (
        mine + node_recv[0].astype(F32) + node_recv[1].astype(F32) + node_recv[2].astype(F32)
    ).astype(BF)

    most = sums_ref.at[c, pl.ds(0, CHIPS - 1)]
    remote(most, most, ssem.at[5], rsem.at[5], sibling).wait_recv()
    share = remote(sums_ref.at[c], sums_ref.at[c], ssem.at[6], rsem.at[6], sibling)
    share.start()

    three = node_send.at[pl.ds(0, 3)]
    remote(patch.at[pl.ds(0, 3)], patch.at[pl.ds(0, 3)], ssem.at[0], rsem.at[0], sibling).wait_send()
    blocks = pl.ds(1, NDEV - 1)
    remote(over_send.at[blocks], over_recv.at[blocks], ssem.at[1], rsem.at[1], sibling).wait_send()
    remote(main_send.at[blocks], main_recv.at[blocks], main_ssem.at[0], main_rsem.at[0], sibling).wait_send()
    remote(three, node_recv, ssem.at[2], rsem.at[2], sibling).wait_send()
    pair.wait_send()
    scattered.wait_send()
    ring.wait_send()
    remote(most, most, ssem.at[5], rsem.at[5], sibling).wait_send()
    share.wait()


def final_kernel(
    sums_in,
    proj_in,
    w_mesh_in,
    w_msg_in,
    w_out_in,
    node_ref,
    mesh_ref,
    grid_ref,
    msg_ref,
    out_ref,
    sums_ref,
    proj_ref,
    w_mesh_ref,
    w_msg_ref,
    w_out_ref,
    load_sem,
):
    loads = [
        pltpu.make_async_copy(src, dst, load_sem.at[k])
        for k, (src, dst) in enumerate(
            (
                (sums_in, sums_ref),
                (proj_in, proj_ref),
                (w_mesh_in, w_mesh_ref),
                (w_msg_in, w_msg_ref),
                (w_out_in, w_out_ref),
            )
        )
    ]
    for load in loads:
        load.start()
    for load in loads:
        load.wait()
    node_ref[...] = dot(proj_ref[...], w_mesh_ref[...], NT).astype(BF)
    mesh_ref[...] = sums_ref[0, :, :, 0:512].astype(F32).reshape(512, 512)
    grid_ref[...] = sums_ref[1, :, :, 0:512].astype(F32).reshape(512, 512)
    low = sums_ref[0, :, :, 512:640].astype(F32).reshape(512, 128)
    high = sums_ref[1, :, :, 512:640].astype(F32).reshape(512, 128)
    moment = jnp.concatenate([low, high], axis=1)[:, 0:227].astype(BF)
    msg_ref[...] = dot(moment, w_out_ref[...], NN)
    out_ref[...] = dot(moment, w_msg_ref[...], TN)


def shards(grad_pred, grid_latent, mesh_latent, send_slot, edge_src, w_mesh, w_grid, w_msg, w_out):
    vmem = pltpu.VMEM
    w_out = w_out.T
    hbm = pl.BlockSpec(memory_space=pltpu.HBM)
    sums, proj = pl.pallas_call(
        kernel,
        in_specs=[hbm] * 9,
        out_shape=[
            jax.ShapeDtypeStruct((2, CHIPS, 8, 640), BF),
            jax.ShapeDtypeStruct((320, 512), BF),
        ],
        scratch_shapes=[
            vmem((227, 768), BF),
            vmem((768, 512), BF),
            vmem((768,), jnp.int32),
            vmem((3, SLOTS), jnp.int32),
            vmem((512, 512), BF),
            vmem((512, 512), BF),
            vmem((512, 512), BF),
            vmem((227, 512), BF),
            pltpu.SemaphoreType.DMA((9,)),
            vmem((GROUPS, 8, ROWS), jnp.int32),
            vmem((GROUPS, 3, ROWS, 512), BF),
            vmem((256, 768), BF),
            vmem((NDEV, MAIN, 768), BF),
            vmem((NDEV, OVER, 768), BF),
            vmem((NDEV, MAIN, 768), BF),
            vmem((NDEV, OVER, 768), BF),
            vmem((4, 320, 512), BF),
            vmem((1280, 512), BF),
            vmem((512, 256), BF),
            vmem((1280, 512), F32),
            vmem((4, 320, 512), BF),
            vmem((3, 320, 512), BF),
            vmem((ROWS, 768), BF),
            vmem((3 * ROWS, 512), BF),
            vmem((2, 512, 640), F32),
            vmem((512, 640), F32),
            vmem((16, 32, 640), BF),
            vmem((16, 32, 640), BF),
            vmem((4, 8, 640), BF),
            vmem((3, 8, 640), BF),
            vmem((8, 640), BF),
            pltpu.SemaphoreType.DMA((1,)),
            pltpu.SemaphoreType.DMA((GROUPS - 1,)),
            pltpu.SemaphoreType.DMA((8,)),
            pltpu.SemaphoreType.DMA((8,)),
        ],
        compiler_params=pltpu.CompilerParams(
            collective_id=0, has_side_effects=True, vmem_limit_bytes=67_043_328
        ),
    )(grad_pred, grid_latent, mesh_latent, send_slot, edge_src, w_mesh, w_grid, w_msg, w_out)
    *grads, out_grad = pl.pallas_call(
        final_kernel,
        out_shape=[
            jax.ShapeDtypeStruct((320, 512), BF),
            jax.ShapeDtypeStruct((512, 512), F32),
            jax.ShapeDtypeStruct((512, 512), F32),
            jax.ShapeDtypeStruct((512, 512), F32),
            jax.ShapeDtypeStruct((227, 512), F32),
        ],
        in_specs=[hbm] * 5,
        scratch_shapes=[
            vmem((2, CHIPS, 8, 640), BF),
            vmem((320, 512), BF),
            vmem((512, 512), BF),
            vmem((512, 512), BF),
            vmem((227, 512), BF),
            pltpu.SemaphoreType.DMA((5,)),
        ],
        compiler_params=pltpu.CompilerParams(vmem_limit_bytes=67_043_328),
    )(sums, proj, w_mesh, w_msg, w_out)
    return *grads, out_grad.T


def solution(mesh):
    both = ("band", "sub")
    placed = (P(None, both), P(both, None), P(both, None), P(both), P(None, both))
    return jax.shard_map(
        shards,
        mesh=mesh,
        in_specs=placed + (P(),) * 4,
        out_specs=(P(both, None), P(), P(), P(), P()),
        check_vma=False,
    )
```

```python
import functools
import math

import jax
import jax.numpy as jnp
from jax import lax
from jax.experimental import pallas as pl
from jax.experimental.pallas import tpu as pltpu
from jax.sharding import PartitionSpec as P

MESH = pl.DeviceIdType.MESH
BF, F32 = jnp.bfloat16, jnp.float32
MAIN, OVER = 16, 2
CAP = MAIN + OVER
NDEV = 128
NN = (((1,), (0,)), ((), ()))
NT = (((1,), (1,)), ((), ()))
TN = (((0,), (0,)), ((), ()))
MIX, UNMIX = 13, 5


def dot(a, b, dims):
    return lax.dot_general(a, b, dims, preferred_element_type=F32)


def place():
    band, sub = lax.axis_index("band"), lax.axis_index("sub")
    return lax.div(band, 8), lax.rem(lax.div(band, 2), 4), lax.rem(band, 2), sub


def shifted(u, dy):
    z, x, c, y = place()
    z = lax.rem(z + lax.rem(u, 4), 4)
    x = lax.rem(x + lax.rem(lax.div(u, 4), 4), 4)
    c = lax.rem(c + lax.div(u, 16), 2)
    return z * 8 + x * 2 + c, lax.rem(y + dy, 4)


def near(d):
    return shifted(lax.rem(d * MIX, 32), 0)


def beside(d):
    t = d - 32
    return shifted(lax.rem(lax.div(t, 2) * MIX, 32), 1 + 2 * lax.rem(t, 2))


def opposite(d):
    return shifted(lax.rem((d - 96) * MIX, 32), 2)


def source(d):
    z, x, c, y = place()
    q = jnp.where(d < 32, d, jnp.where(d < 96, (d - 32) >> 1, d - 96))
    u = (q * MIX) & 31
    dy = jnp.where(d < 32, 0, jnp.where(d < 96, 1 + 2 * (d & 1), 2))
    band = ((z - u) & 3) * 8 + ((x - (u >> 2)) & 3) * 2 + ((c - (u >> 4)) & 1)
    return band * 4 + ((y - dy) & 3)


ROWS = 256
GROUPS = NDEV * CAP // ROWS
BLOCKS = ROWS // MAIN
SLOTS = NDEV * CAP


def plane_peer(q):
    z, x, c, y = place()
    p = lax.rem(q * 5, 16)
    z = lax.rem(z + lax.div(p, 4), 4)
    x = lax.rem(x + lax.rem(p, 4), 4)
    return (z * 8 + x * 2 + c, y), z * 4 + x


def remote(src, dst, send, recv, device):
    return pltpu.make_async_remote_copy(
        src_ref=src,
        dst_ref=dst,
        send_sem=send,
        recv_sem=recv,
        device_id=device,
        device_id_type=MESH,
    )


def kernel(
    grad_in,
    latent_in,
    mesh_in,
    slot_in,
    edge_in,
    w_mesh_in,
    w_grid_in,
    w_msg_in,
    w_out_in,
    outer_ref,
    inner_ref,
    proj_ref,
    grad_ref,
    latent_ref,
    slot_ref,
    edge_ref,
    w_mesh_ref,
    w_grid_ref,
    w_msg_ref,
    w_out_ref,
    load_sem,
    index_ref,
    gathered,
    weighted,
    main_send,
    over_send,
    main_recv,
    over_recv,
    patch,
    table,
    back,
    node,
    node_send,
    node_recv,
    rows_ref,
    outer_part,
    outer_pair,
    outer_rs_send,
    outer_rs_recv,
    outer_ring_send,
    outer_ring_recv,
    inner_part,
    inner_pair,
    inner_rs_send,
    inner_rs_recv,
    inner_ring_send,
    inner_ring_recv,
    psem,
    qsem,
    main_ssem,
    main_rsem,
    ssem,
    rsem,
):
    z, x, c, y = place()
    band = lax.axis_index("band")
    sibling = (band + 1 - 2 * c, y)
    loads = [
        pltpu.make_async_copy(src, dst, load_sem.at[k])
        for k, (src, dst) in enumerate(
            (
                (grad_in, grad_ref),
                (slot_in, slot_ref),
                (latent_in, latent_ref),
                (mesh_in, patch.at[y]),
                (edge_in, edge_ref),
                (w_msg_in, w_msg_ref),
                (w_out_in, w_out_ref),
                (w_mesh_in, w_mesh_ref),
                (w_grid_in, w_grid_ref),
            )
        )
    ]
    for load in loads:
        load.start()
    bar = pltpu.get_barrier_semaphore()

    def each(peer, act):
        def run(d, carry):
            act(d, peer(d))
            return carry

        return run

    def greet(d, device):
        pl.semaphore_signal(bar, inc=1, device_id=device, device_id_type=MESH)

    lax.fori_loop(1, 32, each(near, greet), 0)
    lax.fori_loop(32, 96, each(beside, greet), 0)
    lax.fori_loop(96, NDEV, each(opposite, greet), 0)
    loads[3].wait()
    pl.semaphore_wait(bar, NDEV - 1)
    above, below = lax.rem(y + 1, 4), lax.rem(y + 3, 4)
    half = pl.ds(0, 160)
    rest = pl.ds(160, 160)

    def patch_copy(n, block, to):
        return remote(block, block, psem.at[n], qsem.at[n], (band, to))

    up = patch_copy(0, patch.at[y], above)
    down = patch_copy(1, patch.at[y], below)
    up_half = patch_copy(2, patch.at[below, rest], above)
    down_half = patch_copy(3, patch.at[above, half], below)
    up.start()
    down.start()
    for k in (0, 1, 2, 4, 5, 6, 7, 8):
        loads[k].wait()
    channels, points = grad_ref.shape
    me = band * 4 + y
    lane = lax.broadcasted_iota(jnp.int32, (1, points), 1)
    total = points * NDEV
    angle = jnp.pi * (((me * points + lane).astype(F32) + 0.5) / total - 0.5)
    weight = 0.5 * jnp.pi * jnp.cos(angle)
    weighted[...] = jnp.zeros_like(weighted)
    weighted[0:channels, :] = (weight * grad_ref[...].astype(F32)).astype(BF)
    slot = slot_ref[...].reshape(1, points)
    j = (slot * 3641) >> 16
    r = slot - j * CAP
    dy = (j - y) & 3
    u = (((j >> 5) - z) & 3) + 4 * (((j >> 3) - x) & 3) + 16 * (((j >> 2) - c) & 1)
    q = (u * UNMIX) & 31
    d = jnp.where(dy == 0, q, jnp.where(dy == 2, 96 + q, 32 + 2 * q + (dy >> 1)))
    at_main = jnp.where(r < MAIN, d * MAIN + r, -1)
    at_over = jnp.where(r >= MAIN, d * OVER + r - MAIN, -1)
    row = lax.broadcasted_iota(jnp.int32, (ROWS, points), 0)

    def pick(at, base):
        hot = jnp.where(row == at - base, 1.0, 0.0).astype(BF)
        lat = dot(hot, latent_ref[...], NN).astype(BF)
        gr = dot(hot, weighted[...], NT).astype(BF)
        return lat, gr

    lat, gr = pick(at_over, 0)
    over_send[:, :, 0:512] = lat.reshape(NDEV, OVER, 512)
    over_send[:, :, 512:768] = gr.reshape(NDEV, OVER, 256)
    over_recv[0] = over_send[0]

    def pick_main(g):
        lat, gr = pick(at_main, g * ROWS)
        blocks = pl.ds(g * BLOCKS, BLOCKS)
        main_send[blocks, :, 0:512] = lat.reshape(BLOCKS, MAIN, 512)
        main_send[blocks, :, 512:768] = gr.reshape(BLOCKS, MAIN, 256)

    def send_over(d, device):
        remote(
            over_send.at[d], over_recv.at[d], ssem.at[1], rsem.at[1], device
        ).start()

    def send_main(d, device):
        remote(
            main_send.at[d],
            main_recv.at[d],
            main_ssem.at[0],
            main_rsem.at[lax.div(d, BLOCKS)],
            device,
        ).start()

    pick_main(0)
    pick_main(1)
    main_recv[0] = main_send[0]
    lax.fori_loop(1, 32, each(near, send_main), 0)
    lax.fori_loop(1, 32, each(near, send_over), 0)

    def prep_group(g, carry):
        pick_main(g)
        return carry

    lax.fori_loop(2, GROUPS - 1, prep_group, 0)
    up.wait_recv()
    up_half.start()
    down.wait_recv()
    down_half.start()
    back[...] = jnp.zeros_like(back)
    back[:, 0:channels] = dot(w_msg_ref[...], w_out_ref[...], NT).astype(BF)
    node[...] = jnp.zeros_like(node)
    outer_part[...] = jnp.zeros_like(outer_part)

    size = table.shape[0]
    local = edge_ref[...] - band * size
    halves = jnp.concatenate(
        [(local >> 4).astype(F32), (local & 15).astype(F32), jnp.zeros((2, SLOTS), F32)], axis=0
    ).astype(BF)
    lanes = lax.broadcasted_iota(jnp.int32, (ROWS, SLOTS), 1)
    line = lax.broadcasted_iota(jnp.int32, (ROWS, 1), 0)

    def find(g, slots):
        hot = jnp.where(lanes == slots, 1.0, 0.0).astype(BF)
        found = dot(halves, hot, NT)
        whole = (found[0:3] * 16.0 + found[3:6]).astype(jnp.int32)
        index_ref[g, 0:3, :] = whole

    def find_main(g, carry):
        find(g, source((g - 1) * BLOCKS + (line >> 4)) * CAP + (line & 15))
        return carry

    index_ref[...] = jnp.zeros_like(index_ref)
    find(0, source(line >> 1) * CAP + MAIN + (line & 1))
    lax.fori_loop(1, GROUPS, find_main, 0)

    up_half.wait_recv()
    down_half.wait_recv()
    lax.fori_loop(32, 96, each(beside, send_over), 0)
    lax.fori_loop(96, NDEV, each(opposite, send_over), 0)
    lax.fori_loop(32, 96, each(beside, send_main), 0)
    lax.fori_loop(96, NDEV, each(opposite, send_main), 0)
    for k in range(4):
        table[pl.ds(k * 320, 320), :] = dot(patch[k], w_mesh_ref[...], NN).astype(BF)

    def collect(g, carry):
        column = index_ref[g].T
        node_col = lax.broadcasted_iota(jnp.int32, (ROWS, size), 1)
        for k in range(3):
            hot = jnp.where(node_col == column[:, k : k + 1], 1.0, 0.0).astype(BF)
            gathered[g, k] = dot(hot, table[...], NN).astype(BF)
        return carry

    lax.fori_loop(0, GROUPS, collect, 0)

    def group(g):
        latent, grad = rows_ref[:, 0:512], rows_ref[:, 512:768]
        grid_proj = dot(latent, w_grid_ref[...], NN).astype(BF).astype(F32)
        act_grad = dot(grad, back[...], NT)
        act = jnp.zeros((ROWS, 512), F32)
        total = jnp.zeros((ROWS, 512), F32)
        for k in range(3):
            pre = gathered[g, k].astype(F32) + grid_proj
            sigma = 0.5 * jnp.tanh(0.5 * pre) + 0.5
            value = pre * sigma
            act += value
            grad_k = (act_grad * (sigma + value * (1.0 - sigma))).astype(BF)
            total += grad_k.astype(F32)
            gathered[g, k] = grad_k
        act = act.astype(BF)
        moment = dot(act, grad, TN)
        across = dot(latent, total.astype(BF), TN)
        for h in range(2):
            outer_part[h, :, 0:256] += across[:, h * 256 : h * 256 + 256]
            outer_part[h, :, 256:384] += moment[:, h * 128 : h * 128 + 128]

    def spread(g):
        index = index_ref[g]
        node_row = lax.broadcasted_iota(jnp.int32, (size, ROWS), 0)
        hots = [
            jnp.where(node_row == index[k : k + 1, :], 1.0, 0.0).astype(BF)
            for k in range(3)
        ]
        values = gathered[g].reshape(3 * ROWS, 512)
        node[...] += dot(jnp.concatenate(hots, axis=1), values, NN)

    def await_main(g, first, count):
        blocks = pl.ds(first, count)
        remote(
            main_send.at[blocks], main_recv.at[blocks], main_ssem.at[0], main_rsem.at[g], sibling
        ).wait_recv()

    def load_main(g):
        blocks = pl.ds(g * BLOCKS, BLOCKS)
        rows_ref[...] = main_recv[blocks, :, :].reshape(ROWS, 768)

    def turn(i):
        return jnp.where(i < 2, i + 1, jnp.where(i == 2, 0, i))

    def step(i, carry):
        @pl.when(i > 0)
        def _():
            spread(turn(i - 1))

        @pl.when(i == 0)
        def _():
            await_main(0, 1, BLOCKS - 1)
            load_main(0)

        @pl.when(i == 1)
        def _():
            await_main(1, BLOCKS, BLOCKS)
            load_main(1)

        @pl.when(i == 2)
        def _():
            blocks = pl.ds(1, NDEV - 1)
            remote(
                over_send.at[blocks], over_recv.at[blocks], ssem.at[1], rsem.at[1], sibling
            ).wait_recv()
            rows_ref[...] = over_recv[...].reshape(ROWS, 768)

        @pl.when(i > 2)
        def _():
            await_main(i - 1, (i - 1) * BLOCKS, BLOCKS)
            load_main(i - 1)

        group(turn(i))
        return carry

    lax.fori_loop(0, GROUPS, step, 0)

    plane = z * 4 + x
    scale = 1.0 / math.sqrt(3.0 * points * NDEV)

    def chain(base, part, pair_recv, rs_send, rs_recv, ring_send, ring_recv, sums):
        width = part.shape[2]

        def lane(n):
            return ssem.at[base + n], rsem.at[base + n]

        pair = remote(part.at[1 - c], pair_recv, *lane(0), sibling)
        others = pl.ds(1, 15)
        scattered = remote(rs_send.at[others], rs_recv.at[others], *lane(1), sibling)
        three = ring_send.at[pl.ds(0, 3)]
        ringed = remote(three, ring_recv, *lane(2), sibling)
        lifted = sums.at[c, plane, pl.ds(0, 3)]
        lifted = remote(lifted, lifted, *lane(3), sibling)
        most = sums.at[c, pl.ds(0, 15)]
        spread_out = remote(most, most, *lane(4), sibling)
        share = remote(sums.at[c], sums.at[c], *lane(5), sibling)

        def scatter():
            pair.wait_recv()
            rs_send[...] = (part[c] + pair_recv[...]).astype(BF).reshape(16, 32, width)

            def send(q, carry):
                device, to = plane_peer(q)
                remote(rs_send.at[to], rs_recv.at[q], *lane(1), device).start()
                return carry

            lax.fori_loop(1, 16, send, 0)
            rs_recv[0] = rs_send[plane]

        def ring():
            scattered.wait_recv()
            whole = rs_recv[0].astype(F32)
            for k in range(1, 16):
                whole += rs_recv[k].astype(F32)
            ring_send[...] = whole.astype(BF).reshape(4, 8, width)
            for k in (1, 2, 3):
                to = lax.rem(y + k, 4)
                remote(ring_send.at[to], ring_recv.at[k - 1], *lane(2), (band, to)).start()

        def lift():
            ringed.wait_recv()
            whole = ring_send[y].astype(F32)
            for k in range(3):
                whole += ring_recv[k].astype(F32)
            sums[c, plane, y] = (whole * scale).astype(BF)
            block = sums.at[c, plane, y]
            for k in (1, 2, 3):
                remote(block, block, *lane(3), (band, lax.rem(y + k, 4))).start()

        def gather():
            lifted.wait_recv()
            block = sums.at[c, plane]

            def send(q, carry):
                device, _ = plane_peer(q)
                remote(block, block, *lane(4), device).start()
                return carry

            lax.fori_loop(1, 16, send, 0)

        def swap():
            spread_out.wait_recv()
            share.start()

        def drain():
            for copy in (pair, scattered, ringed, lifted, spread_out):
                copy.wait_send()
            share.wait()

        return pair, scatter, ring, lift, gather, swap, drain

    a_pair, a_scatter, a_ring, a_lift, a_gather, a_swap, a_drain = chain(
        4, outer_part, outer_pair, outer_rs_send, outer_rs_recv, outer_ring_send, outer_ring_recv, outer_ref
    )
    b_pair, b_scatter, b_ring, b_lift, b_gather, b_swap, b_drain = chain(
        10, inner_part, inner_pair, inner_rs_send, inner_rs_recv, inner_ring_send, inner_ring_recv, inner_ref
    )

    def node_send_half(n, rows):
        for k in (1, 2, 3):
            to = lax.rem(y + k, 4)
            remote(
                node_send.at[to, rows], node_recv.at[k - 1, rows], ssem.at[n], rsem.at[n], (band, to)
            ).start()

    def node_wait(n, rows):
        return remote(
            node_send.at[pl.ds(0, 3), rows], node_recv.at[:, rows], ssem.at[n], rsem.at[n], sibling
        )

    a_pair.start()
    spread(GROUPS - 1)
    for k in range(4):
        node_send[k] = node[pl.ds(k * 320, 320), :].astype(BF)
    a_scatter()
    node_send_half(2, half)
    across = dot(patch[0], node_send[0], TN)
    for k in (1, 2, 3):
        across += dot(patch[k], node_send[k], TN)
    for h in range(2):
        inner_part[h] = across[:, h * 256 : h * 256 + 256]
    b_pair.start()
    b_scatter()
    a_ring()
    b_ring()
    a_lift()
    b_lift()
    node_send_half(3, rest)
    a_gather()
    b_gather()
    first, second = node_wait(2, half), node_wait(3, rest)
    first.wait_recv()
    second.wait_recv()
    mine = node[pl.ds(y * 320, 320), :]
    proj_ref[...] = (
        mine + node_recv[0].astype(F32) + node_recv[1].astype(F32) + node_recv[2].astype(F32)
    ).astype(BF)
    a_swap()
    b_swap()

    for copy in (up, down, up_half, down_half, first, second):
        copy.wait_send()
    blocks = pl.ds(1, NDEV - 1)
    remote(over_send.at[blocks], over_recv.at[blocks], ssem.at[1], rsem.at[1], sibling).wait_send()
    remote(main_send.at[blocks], main_recv.at[blocks], main_ssem.at[0], main_rsem.at[0], sibling).wait_send()
    a_drain()
    b_drain()


def final_kernel(*refs):
    ins, outs, held, done, sems = refs[0:6], refs[6:11], refs[11:17], refs[17:22], refs[22]
    loads = [
        pltpu.make_async_copy(src, dst, sems.at[k])
        for k, (src, dst) in enumerate(zip(ins, held))
    ]
    for load in loads:
        load.start()
    stores = [
        pltpu.make_async_copy(src, dst, sems.at[6 + k])
        for k, (src, dst) in enumerate(zip(done, outs))
    ]
    outer_ref, inner_ref, proj_ref, w_mesh_ref, w_msg_ref, w_out_ref = held
    node_ref, mesh_ref, grid_ref, msg_ref, out_ref = done
    loads[1].wait()
    for h in range(2):
        mesh_ref[:, h * 256 : h * 256 + 256] = inner_ref[h].astype(F32).reshape(512, 256)
    stores[1].start()
    loads[0].wait()
    moment = []
    for h in range(2):
        whole = outer_ref[h].astype(F32).reshape(512, 384)
        grid_ref[:, h * 256 : h * 256 + 256] = whole[:, 0:256]
        moment.append(whole[:, 256:384])
    stores[2].start()
    moment = jnp.concatenate(moment, axis=1)[:, 0:227].astype(BF)
    loads[5].wait()
    msg_ref[...] = dot(moment, w_out_ref[...], NN)
    stores[3].start()
    loads[4].wait()
    out_ref[...] = dot(moment, w_msg_ref[...], TN)
    stores[4].start()
    loads[2].wait()
    loads[3].wait()
    node_ref[...] = dot(proj_ref[...], w_mesh_ref[...], NT).astype(BF)
    stores[0].start()
    for store in stores:
        store.wait()


def shards(grad_pred, grid_latent, mesh_latent, send_slot, edge_src, w_mesh, w_grid, w_msg, w_out):
    vmem = pltpu.VMEM
    w_out = w_out.T
    hbm = pl.BlockSpec(memory_space=pltpu.HBM)
    outer, inner, proj = pl.pallas_call(
        kernel,
        in_specs=[hbm] * 9,
        out_shape=[
            jax.ShapeDtypeStruct((2, 16, 4, 8, 384), BF),
            jax.ShapeDtypeStruct((2, 16, 4, 8, 256), BF),
            jax.ShapeDtypeStruct((320, 512), BF),
        ],
        scratch_shapes=[
            vmem((227, 768), BF),
            vmem((768, 512), BF),
            vmem((768,), jnp.int32),
            vmem((3, SLOTS), jnp.int32),
            vmem((512, 512), BF),
            vmem((512, 512), BF),
            vmem((512, 512), BF),
            vmem((227, 512), BF),
            pltpu.SemaphoreType.DMA((9,)),
            vmem((GROUPS, 8, ROWS), jnp.int32),
            vmem((GROUPS, 3, ROWS, 512), BF),
            vmem((256, 768), BF),
            vmem((NDEV, MAIN, 768), BF),
            vmem((NDEV, OVER, 768), BF),
            vmem((NDEV, MAIN, 768), BF),
            vmem((NDEV, OVER, 768), BF),
            vmem((4, 320, 512), BF),
            vmem((1280, 512), BF),
            vmem((512, 256), BF),
            vmem((1280, 512), F32),
            vmem((4, 320, 512), BF),
            vmem((3, 320, 512), BF),
            vmem((ROWS, 768), BF),
            vmem((2, 512, 384), F32),
            vmem((512, 384), F32),
            vmem((16, 32, 384), BF),
            vmem((16, 32, 384), BF),
            vmem((4, 8, 384), BF),
            vmem((3, 8, 384), BF),
            vmem((2, 512, 256), F32),
            vmem((512, 256), F32),
            vmem((16, 32, 256), BF),
            vmem((16, 32, 256), BF),
            vmem((4, 8, 256), BF),
            vmem((3, 8, 256), BF),
            pltpu.SemaphoreType.DMA((4,)),
            pltpu.SemaphoreType.DMA((4,)),
            pltpu.SemaphoreType.DMA((1,)),
            pltpu.SemaphoreType.DMA((GROUPS - 1,)),
            pltpu.SemaphoreType.DMA((16,)),
            pltpu.SemaphoreType.DMA((16,)),
        ],
        compiler_params=pltpu.CompilerParams(
            collective_id=0, has_side_effects=True, vmem_limit_bytes=67_043_328
        ),
    )(grad_pred, grid_latent, mesh_latent, send_slot, edge_src, w_mesh, w_grid, w_msg, w_out)
    shapes = [
        ((320, 512), BF),
        ((512, 512), F32),
        ((512, 512), F32),
        ((512, 512), F32),
        ((227, 512), F32),
    ]
    operands = (outer, inner, proj, w_mesh, w_msg, w_out)
    *grads, out_grad = pl.pallas_call(
        final_kernel,
        out_shape=[jax.ShapeDtypeStruct(*shape) for shape in shapes],
        in_specs=[hbm] * 6,
        out_specs=[hbm] * 5,
        scratch_shapes=[
            *(vmem(operand.shape, BF) for operand in operands),
            *(vmem(*shape) for shape in shapes),
            pltpu.SemaphoreType.DMA((11,)),
        ],
        compiler_params=pltpu.CompilerParams(vmem_limit_bytes=67_043_328),
    )(*operands)
    return *grads, out_grad.T


def solution(mesh):
    both = ("band", "sub")
    placed = (P(None, both), P(both, None), P(both, None), P(both), P(None, both))
    return jax.shard_map(
        shards,
        mesh=mesh,
        in_specs=placed + (P(),) * 4,
        out_specs=(P(both, None), P(), P(), P(), P()),
        check_vma=False,
    )
```

```python
import functools
import math

import jax
import jax.numpy as jnp
from jax import lax
from jax.experimental import pallas as pl
from jax.experimental.pallas import tpu as pltpu
from jax.sharding import PartitionSpec as P

MESH = pl.DeviceIdType.MESH
BF, F32 = jnp.bfloat16, jnp.float32
MAIN, OVER = 16, 2
CAP = MAIN + OVER
NDEV = 128
NN = (((1,), (0,)), ((), ()))
NT = (((1,), (1,)), ((), ()))
TN = (((0,), (0,)), ((), ()))


def dot(a, b, dims):
    return lax.dot_general(a, b, dims, preferred_element_type=F32)


def place():
    band, sub = lax.axis_index("band"), lax.axis_index("sub")
    return lax.div(band, 8), lax.rem(lax.div(band, 2), 4), lax.rem(band, 2), sub


def source(d):
    z, x, c, y = place()
    q = jnp.where(d < 32, d, jnp.where(d < 96, (d - 32) >> 1, d - 96))
    dy = jnp.where(d < 32, 0, jnp.where(d < 96, 1 + 2 * (d & 1), 2))
    i, o = q & 7, q >> 3
    band = ((z - o - i) & 3) * 8 + ((x - i) & 3) * 2 + ((c - (i >> 2)) & 1)
    return band * 4 + ((y - dy) & 3)


ROWS = 256
GROUPS = NDEV * CAP // ROWS
BLOCKS = ROWS // MAIN
SLOTS = NDEV * CAP


def remote(src, dst, send, recv, device):
    return pltpu.make_async_remote_copy(
        src_ref=src,
        dst_ref=dst,
        send_sem=send,
        recv_sem=recv,
        device_id=device,
        device_id_type=MESH,
    )


def kernel(
    grad_in,
    latent_in,
    mesh_in,
    slot_in,
    edge_in,
    w_mesh_in,
    w_grid_in,
    w_msg_in,
    w_out_in,
    outer_ref,
    inner_ref,
    proj_ref,
    grad_ref,
    latent_ref,
    slot_ref,
    edge_ref,
    w_mesh_ref,
    w_grid_ref,
    w_msg_ref,
    w_out_ref,
    load_sem,
    index_ref,
    gathered,
    weighted,
    main_send,
    over_send,
    main_recv,
    over_recv,
    patch,
    patch_t,
    table,
    back,
    node,
    node_send,
    node_recv,
    rows_ref,
    outer_part,
    outer_pair,
    outer_rs_send,
    outer_rs_recv,
    outer_ring,
    inner_part,
    inner_pair,
    inner_rs_send,
    inner_rs_recv,
    inner_ring,
    psem,
    qsem,
    main_ssem,
    main_rsem,
    ssem,
    rsem,
):
    z, x, c, y = place()
    band = lax.axis_index("band")
    sibling = (band + 1 - 2 * c, y)
    above, below = lax.rem(y + 1, 4), lax.rem(y + 3, 4)
    loads = [
        pltpu.make_async_copy(src, dst, load_sem.at[k])
        for k, (src, dst) in enumerate(
            (
                (grad_in, grad_ref),
                (slot_in, slot_ref),
                (latent_in, latent_ref),
                (mesh_in, patch.at[y]),
                (edge_in, edge_ref),
                (w_msg_in, w_msg_ref),
                (w_out_in, w_out_ref),
                (w_mesh_in, w_mesh_ref),
                (w_grid_in, w_grid_ref),
            )
        )
    ]
    for load in loads:
        load.start()
    bar = pltpu.get_barrier_semaphore()

    def greet(n, carry):
        to = band + n
        to = jnp.where(to < 32, to, to - 32)
        for k in range(4):
            pl.semaphore_signal(bar, inc=1, device_id=(to, k), device_id_type=MESH)
        return carry

    for k in (1, 2, 3):
        pl.semaphore_signal(
            bar, inc=1, device_id=(band, lax.rem(y + k, 4)), device_id_type=MESH
        )
    lax.fori_loop(1, 32, greet, 0)

    columns = [lax.rem(x + k, 4) * 2 for k in range(4)]
    cores = [c, 1 - c]
    cross = lax.rem(y + 2, 4)

    def bands(o, first=0):
        for i in range(first, 8):
            yield o * 8 + i, lax.rem(z + o + i, 4) * 8 + columns[i % 4] + cores[i // 4]

    def near(act):
        for v, to in bands(0, 1):
            act(v, (to, y))

        def run(o, carry):
            for v, to in bands(o):
                act(v, (to, y))
            return carry

        lax.fori_loop(1, 4, run, 0)

    def far(act):
        def beside(o, carry):
            for v, to in bands(o):
                act(32 + 2 * v, (to, above))
                act(33 + 2 * v, (to, below))
            return carry

        def opposite(o, carry):
            for v, to in bands(o):
                act(96 + v, (to, cross))
            return carry

        lax.fori_loop(0, 4, beside, 0)
        lax.fori_loop(0, 4, opposite, 0)

    loads[3].wait()
    pl.semaphore_wait(bar, NDEV - 1)
    half = pl.ds(0, 160)
    rest = pl.ds(160, 160)

    def patch_copy(n, block, to):
        return remote(block, block, psem.at[n], qsem.at[n], (band, to))

    up = patch_copy(0, patch.at[y], above)
    down = patch_copy(1, patch.at[y], below)
    up_half = patch_copy(2, patch.at[below, rest], above)
    down_half = patch_copy(3, patch.at[above, half], below)
    up.start()
    down.start()
    for k in (0, 1, 2, 4, 5, 6, 7, 8):
        loads[k].wait()
    channels, points = grad_ref.shape
    me = band * 4 + y
    lane = lax.broadcasted_iota(jnp.int32, (1, points), 1)
    total = points * NDEV
    angle = jnp.pi * (((me * points + lane).astype(F32) + 0.5) / total - 0.5)
    weight = 0.5 * jnp.pi * jnp.cos(angle)
    weighted[...] = jnp.zeros_like(weighted)
    weighted[0:channels, :] = (weight * grad_ref[...].astype(F32)).astype(BF)
    slot = slot_ref[...].reshape(1, points)
    j = (slot * 3641) >> 16
    r = slot - j * CAP
    dy = (j - y) & 3
    i = (((j >> 3) - x) & 3) + 4 * (((j >> 2) - c) & 1)
    q = 8 * ((((j >> 5) - z) - i) & 3) + i
    d = jnp.where(dy == 0, q, jnp.where(dy == 2, 96 + q, 32 + 2 * q + (dy >> 1)))
    at_main = jnp.where(r < MAIN, d * MAIN + r, -1)
    at_over = jnp.where(r >= MAIN, d * OVER + r - MAIN, -1)
    row = lax.broadcasted_iota(jnp.int32, (ROWS, points), 0)

    def pick(at, base):
        hot = jnp.where(row == at - base, 1.0, 0.0).astype(BF)
        lat = dot(hot, latent_ref[...], NN).astype(BF)
        gr = dot(hot, weighted[...], NT).astype(BF)
        return lat, gr

    lat, gr = pick(at_over, 0)
    over_send[:, :, 0:512] = lat.reshape(NDEV, OVER, 512)
    over_send[:, :, 512:768] = gr.reshape(NDEV, OVER, 256)
    over_recv[0] = over_send[0]

    def pick_main(g):
        lat, gr = pick(at_main, g * ROWS)
        blocks = pl.ds(g * BLOCKS, BLOCKS)
        main_send[blocks, :, 0:512] = lat.reshape(BLOCKS, MAIN, 512)
        main_send[blocks, :, 512:768] = gr.reshape(BLOCKS, MAIN, 256)

    def send_over(d, device):
        remote(
            over_send.at[d], over_recv.at[d], ssem.at[1], rsem.at[1], device
        ).start()

    def send_main(d, device):
        remote(
            main_send.at[d],
            main_recv.at[d],
            main_ssem.at[0],
            main_rsem.at[lax.div(d, BLOCKS)],
            device,
        ).start()

    pick_main(0)
    pick_main(1)
    main_recv[0] = main_send[0]
    near(send_main)
    near(send_over)

    def prep_group(g, carry):
        pick_main(g)
        return carry

    lax.fori_loop(2, GROUPS - 1, prep_group, 0)
    up.wait_recv()
    up_half.start()
    down.wait_recv()
    down_half.start()
    up_half.wait_recv()
    down_half.wait_recv()
    far(send_over)
    far(send_main)
    back[...] = jnp.zeros_like(back)
    back[:, 0:channels] = dot(w_msg_ref[...], w_out_ref[...], NT).astype(BF)
    node[...] = jnp.zeros_like(node)
    outer_part[...] = jnp.zeros_like(outer_part)

    size = table.shape[0]
    local = edge_ref[...] - band * size
    halves = jnp.concatenate(
        [(local >> 4).astype(F32), (local & 15).astype(F32), jnp.zeros((2, SLOTS), F32)], axis=0
    ).astype(BF)
    lanes = lax.broadcasted_iota(jnp.int32, (ROWS, SLOTS), 1)
    line = lax.broadcasted_iota(jnp.int32, (ROWS, 1), 0)

    def find(g, slots):
        hot = jnp.where(lanes == slots, 1.0, 0.0).astype(BF)
        found = dot(halves, hot, NT)
        whole = (found[0:3] * 16.0 + found[3:6]).astype(jnp.int32)
        index_ref[g, 0:3, :] = whole

    def find_main(g, carry):
        find(g, source((g - 1) * BLOCKS + (line >> 4)) * CAP + (line & 15))
        return carry

    index_ref[...] = jnp.zeros_like(index_ref)
    find(0, source(line >> 1) * CAP + MAIN + (line & 1))
    lax.fori_loop(1, GROUPS, find_main, 0)

    for k in range(4):
        table[pl.ds(k * 320, 320), :] = dot(patch[k], w_mesh_ref[...], NN).astype(BF)

    def collect(g, carry):
        column = index_ref[g].T
        node_col = lax.broadcasted_iota(jnp.int32, (ROWS, size), 1)
        for k in range(3):
            hot = jnp.where(node_col == column[:, k : k + 1], 1.0, 0.0).astype(BF)
            gathered[g, k] = dot(hot, table[...], NN).astype(BF)
        return carry

    lax.fori_loop(0, GROUPS, collect, 0)
    patch_t[...] = patch[...].reshape(size, 512).T

    def group(g):
        latent, grad = rows_ref[:, 0:512], rows_ref[:, 512:768]
        grid_proj = dot(latent, w_grid_ref[...], NN).astype(BF).astype(F32)
        act_grad = dot(grad, back[...], NT)
        act = jnp.zeros((ROWS, 512), F32)
        total = jnp.zeros((ROWS, 512), F32)
        for k in range(3):
            pre = gathered[g, k].astype(F32) + grid_proj
            sigma = 0.5 * jnp.tanh(0.5 * pre) + 0.5
            value = pre * sigma
            act += value
            grad_k = (act_grad * (sigma + value * (1.0 - sigma))).astype(BF)
            total += grad_k.astype(F32)
            gathered[g, k] = grad_k
        act = act.astype(BF)
        moment = dot(act, grad, TN)
        across = dot(latent, total.astype(BF), TN)
        for h in range(2):
            outer_part[h, :, 0:256] += across[:, h * 256 : h * 256 + 256]
            outer_part[h, :, 256:384] += moment[:, h * 128 : h * 128 + 128]

    def spread(g):
        index = index_ref[g]
        node_row = lax.broadcasted_iota(jnp.int32, (size, ROWS), 0)
        hots = [
            jnp.where(node_row == index[k : k + 1, :], 1.0, 0.0).astype(BF)
            for k in range(3)
        ]
        values = gathered[g].reshape(3 * ROWS, 512)
        node[...] += dot(jnp.concatenate(hots, axis=1), values, NN)

    def await_main(g, first, count):
        blocks = pl.ds(first, count)
        remote(
            main_send.at[blocks], main_recv.at[blocks], main_ssem.at[0], main_rsem.at[g], sibling
        ).wait_recv()

    def load_main(g):
        blocks = pl.ds(g * BLOCKS, BLOCKS)
        rows_ref[...] = main_recv[blocks, :, :].reshape(ROWS, 768)

    def turn(i):
        return jnp.where(i < 2, i + 1, jnp.where(i == 2, 0, i))

    def step(i, carry):
        @pl.when(i > 0)
        def _():
            spread(turn(i - 1))

        @pl.when(i == 0)
        def _():
            await_main(0, 1, BLOCKS - 1)
            load_main(0)

        @pl.when(i == 1)
        def _():
            await_main(1, BLOCKS, BLOCKS)
            load_main(1)

        @pl.when(i == 2)
        def _():
            blocks = pl.ds(1, NDEV - 1)
            remote(
                over_send.at[blocks], over_recv.at[blocks], ssem.at[1], rsem.at[1], sibling
            ).wait_recv()
            rows_ref[...] = over_recv[...].reshape(ROWS, 768)

        @pl.when(i > 2)
        def _():
            await_main(i - 1, (i - 1) * BLOCKS, BLOCKS)
            load_main(i - 1)

        group(turn(i))
        return carry

    lax.fori_loop(0, GROUPS, step, 0)

    plane = z * 4 + x
    planes = []
    for k in range(1, 16):
        n = (5 * k) % 16
        to_z = lax.rem(z + n // 4, 4)
        planes.append(
            (k, (to_z * 8 + columns[n % 4] + c, y), to_z * 4 + lax.rem(x + n % 4, 4))
        )
    scale = 1.0 / math.sqrt(3.0 * points * NDEV)

    def chain(base, part, pair_recv, rs_send, rs_recv, ring, sums):
        width = part.shape[2]

        def lane(n):
            return ssem.at[base + n], rsem.at[base + n]

        pair = remote(part.at[1 - c], pair_recv, *lane(0), sibling)
        others = pl.ds(1, 15)
        scattered = remote(rs_send.at[others], rs_recv.at[others], *lane(1), sibling)
        three = ring.at[pl.ds(0, 3)]
        ringed = remote(three, three, *lane(2), sibling)
        most = sums.at[c, pl.ds(0, 15)]
        spread_out = remote(most, most, *lane(4), sibling)
        share = remote(sums.at[c], sums.at[c], *lane(5), sibling)

        def scatter():
            pair.wait_recv()
            rs_send[...] = (part[c] + pair_recv[...]).astype(BF).reshape(16, 32, width)

            for k, device, to in planes:
                remote(rs_send.at[to], rs_recv.at[k], *lane(1), device).start()
            rs_recv[0] = rs_send[plane]

        def circulate():
            scattered.wait_recv()
            whole = rs_recv[0].astype(F32)
            for k in range(1, 16):
                whole += rs_recv[k].astype(F32)
            ring[y] = whole.astype(BF)
            for k in (1, 2, 3):
                remote(
                    ring.at[y], ring.at[y], *lane(2), (band, lax.rem(y + k, 4))
                ).start()

        def gather():
            ringed.wait_recv()
            whole = ring[0].astype(F32)
            for k in range(1, 4):
                whole += ring[k].astype(F32)
            sums[c, plane] = (whole * scale).astype(BF)
            block = sums.at[c, plane]
            for _, device, _ in planes:
                remote(block, block, *lane(4), device).start()

        def swap():
            spread_out.wait_recv()
            share.start()

        def drain():
            for copy in (pair, scattered, ringed, spread_out):
                copy.wait_send()
            share.wait()

        return pair, scatter, circulate, gather, swap, drain

    a_pair, a_scatter, a_circulate, a_gather, a_swap, a_drain = chain(
        4, outer_part, outer_pair, outer_rs_send, outer_rs_recv, outer_ring, outer_ref
    )
    b_pair, b_scatter, b_circulate, b_gather, b_swap, b_drain = chain(
        10, inner_part, inner_pair, inner_rs_send, inner_rs_recv, inner_ring, inner_ref
    )

    def node_send_half(n, rows):
        for k in (1, 2, 3):
            to = lax.rem(y + k, 4)
            remote(
                node_send.at[to, rows], node_recv.at[k - 1, rows], ssem.at[n], rsem.at[n], (band, to)
            ).start()

    def node_wait(n, rows):
        return remote(
            node_send.at[pl.ds(0, 3), rows], node_recv.at[:, rows], ssem.at[n], rsem.at[n], sibling
        )

    a_pair.start()
    spread(GROUPS - 1)
    node_send[...] = node[...].astype(BF).reshape(4, 320, 512)
    across = dot(patch_t[...], node_send[...].reshape(size, 512), NN)
    for h in range(2):
        inner_part[h] = across[:, h * 256 : h * 256 + 256]
    b_pair.start()
    a_scatter()
    node_send_half(2, half)
    b_scatter()
    a_circulate()
    b_circulate()
    a_gather()
    b_gather()
    node_send_half(3, rest)
    first, second = node_wait(2, half), node_wait(3, rest)
    first.wait_recv()
    second.wait_recv()
    mine = node[pl.ds(y * 320, 320), :]
    proj_ref[...] = (
        mine + node_recv[0].astype(F32) + node_recv[1].astype(F32) + node_recv[2].astype(F32)
    ).astype(BF)
    a_swap()
    b_swap()

    for copy in (up, down, up_half, down_half, first, second):
        copy.wait_send()
    blocks = pl.ds(1, NDEV - 1)
    remote(over_send.at[blocks], over_recv.at[blocks], ssem.at[1], rsem.at[1], sibling).wait_send()
    remote(main_send.at[blocks], main_recv.at[blocks], main_ssem.at[0], main_rsem.at[0], sibling).wait_send()
    a_drain()
    b_drain()


def final_kernel(*refs):
    ins, outs, held, done, sems = refs[0:6], refs[6:11], refs[11:17], refs[17:22], refs[22]
    loads = [
        pltpu.make_async_copy(src, dst, sems.at[k])
        for k, (src, dst) in enumerate(zip(ins, held))
    ]
    for load in loads:
        load.start()
    stores = [
        pltpu.make_async_copy(src, dst, sems.at[6 + k])
        for k, (src, dst) in enumerate(zip(done, outs))
    ]
    outer_ref, inner_ref, proj_ref, w_mesh_ref, w_msg_ref, w_out_ref = held
    node_ref, mesh_ref, grid_ref, msg_ref, out_ref = done
    loads[1].wait()
    for h in range(2):
        mesh_ref[:, h * 256 : h * 256 + 256] = inner_ref[h].astype(F32).reshape(512, 256)
    stores[1].start()
    loads[0].wait()
    moment = []
    for h in range(2):
        whole = outer_ref[h].astype(F32).reshape(512, 384)
        grid_ref[:, h * 256 : h * 256 + 256] = whole[:, 0:256]
        moment.append(whole[:, 256:384])
    stores[2].start()
    moment = jnp.concatenate(moment, axis=1)[:, 0:227].astype(BF)
    loads[5].wait()
    msg_ref[...] = dot(moment, w_out_ref[...], NN)
    stores[3].start()
    loads[4].wait()
    out_ref[...] = dot(moment, w_msg_ref[...], TN)
    stores[4].start()
    loads[2].wait()
    loads[3].wait()
    node_ref[...] = dot(proj_ref[...], w_mesh_ref[...], NT).astype(BF)
    stores[0].start()
    for store in stores:
        store.wait()


def shards(grad_pred, grid_latent, mesh_latent, send_slot, edge_src, w_mesh, w_grid, w_msg, w_out):
    vmem = pltpu.VMEM
    w_out = w_out.T
    hbm = pl.BlockSpec(memory_space=pltpu.HBM)
    outer, inner, proj = pl.pallas_call(
        kernel,
        in_specs=[hbm] * 9,
        out_shape=[
            jax.ShapeDtypeStruct((2, 16, 32, 384), BF),
            jax.ShapeDtypeStruct((2, 16, 32, 256), BF),
            jax.ShapeDtypeStruct((320, 512), BF),
        ],
        scratch_shapes=[
            vmem((227, 768), BF),
            vmem((768, 512), BF),
            vmem((768,), jnp.int32),
            vmem((3, SLOTS), jnp.int32),
            vmem((512, 512), BF),
            vmem((512, 512), BF),
            vmem((512, 512), BF),
            vmem((227, 512), BF),
            pltpu.SemaphoreType.DMA((9,)),
            vmem((GROUPS, 8, ROWS), jnp.int32),
            vmem((GROUPS, 3, ROWS, 512), BF),
            vmem((256, 768), BF),
            vmem((NDEV, MAIN, 768), BF),
            vmem((NDEV, OVER, 768), BF),
            vmem((NDEV, MAIN, 768), BF),
            vmem((NDEV, OVER, 768), BF),
            vmem((4, 320, 512), BF),
            vmem((512, 1280), BF),
            vmem((1280, 512), BF),
            vmem((512, 256), BF),
            vmem((1280, 512), F32),
            vmem((4, 320, 512), BF),
            vmem((3, 320, 512), BF),
            vmem((ROWS, 768), BF),
            vmem((2, 512, 384), F32),
            vmem((512, 384), F32),
            vmem((16, 32, 384), BF),
            vmem((16, 32, 384), BF),
            vmem((4, 32, 384), BF),
            vmem((2, 512, 256), F32),
            vmem((512, 256), F32),
            vmem((16, 32, 256), BF),
            vmem((16, 32, 256), BF),
            vmem((4, 32, 256), BF),
            pltpu.SemaphoreType.DMA((4,)),
            pltpu.SemaphoreType.DMA((4,)),
            pltpu.SemaphoreType.DMA((1,)),
            pltpu.SemaphoreType.DMA((GROUPS - 1,)),
            pltpu.SemaphoreType.DMA((16,)),
            pltpu.SemaphoreType.DMA((16,)),
        ],
        compiler_params=pltpu.CompilerParams(
            collective_id=0, has_side_effects=True, vmem_limit_bytes=67_043_328
        ),
    )(grad_pred, grid_latent, mesh_latent, send_slot, edge_src, w_mesh, w_grid, w_msg, w_out)
    shapes = [
        ((320, 512), BF),
        ((512, 512), F32),
        ((512, 512), F32),
        ((512, 512), F32),
        ((227, 512), F32),
    ]
    operands = (outer, inner, proj, w_mesh, w_msg, w_out)
    *grads, out_grad = pl.pallas_call(
        final_kernel,
        out_shape=[jax.ShapeDtypeStruct(*shape) for shape in shapes],
        in_specs=[hbm] * 6,
        out_specs=[hbm] * 5,
        scratch_shapes=[
            *(vmem(operand.shape, BF) for operand in operands),
            *(vmem(*shape) for shape in shapes),
            pltpu.SemaphoreType.DMA((11,)),
        ],
        compiler_params=pltpu.CompilerParams(vmem_limit_bytes=67_043_328),
    )(*operands)
    return *grads, out_grad.T


def solution(mesh):
    both = ("band", "sub")
    placed = (P(None, both), P(both, None), P(both, None), P(both), P(None, both))
    return jax.shard_map(
        shards,
        mesh=mesh,
        in_specs=placed + (P(),) * 4,
        out_specs=(P(both, None), P(), P(), P(), P()),
        check_vma=False,
    )
```

```python
import functools
import math

import jax
import jax.numpy as jnp
from jax import lax
from jax.experimental import pallas as pl
from jax.experimental.pallas import tpu as pltpu
from jax.sharding import PartitionSpec as P

MESH = pl.DeviceIdType.MESH
BF, F32 = jnp.bfloat16, jnp.float32
MAIN, OVER = 16, 2
CAP = MAIN + OVER
NDEV = 128
NN = (((1,), (0,)), ((), ()))
NT = (((1,), (1,)), ((), ()))
TN = (((0,), (0,)), ((), ()))


def dot(a, b, dims):
    return lax.dot_general(a, b, dims, preferred_element_type=F32)


def place():
    band, sub = lax.axis_index("band"), lax.axis_index("sub")
    return lax.div(band, 8), lax.rem(lax.div(band, 2), 4), lax.rem(band, 2), sub


def source(d):
    z, x, c, y = place()
    q = jnp.where(d < 32, d, jnp.where(d < 96, (d - 32) >> 1, d - 96))
    dy = jnp.where(d < 32, 0, jnp.where(d < 96, 1 + 2 * (d & 1), 2))
    i, o = q & 7, q >> 3
    band = ((z - o - i) & 3) * 8 + ((x - i) & 3) * 2 + ((c - (i >> 2)) & 1)
    return band * 4 + ((y - dy) & 3)


ROWS = 256
GROUPS = NDEV * CAP // ROWS
BLOCKS = ROWS // MAIN
SLOTS = NDEV * CAP


def remote(src, dst, send, recv, device):
    return pltpu.make_async_remote_copy(
        src_ref=src,
        dst_ref=dst,
        send_sem=send,
        recv_sem=recv,
        device_id=device,
        device_id_type=MESH,
    )


def kernel(
    grad_in,
    latent_in,
    mesh_in,
    slot_in,
    edge_in,
    w_mesh_in,
    w_grid_in,
    w_msg_in,
    w_out_in,
    outer_ref,
    inner_ref,
    proj_ref,
    grad_ref,
    latent_ref,
    slot_ref,
    edge_ref,
    w_mesh_ref,
    w_grid_ref,
    w_msg_ref,
    w_out_ref,
    load_sem,
    index_ref,
    gathered,
    weighted,
    main_send,
    over_send,
    main_recv,
    over_recv,
    patch,
    patch_t,
    table,
    back,
    node,
    node_send,
    node_recv,
    rows_ref,
    outer_part,
    outer_pair,
    outer_rs_send,
    outer_rs_recv,
    outer_ring,
    inner_part,
    inner_pair,
    inner_rs_send,
    inner_rs_recv,
    inner_ring,
    psem,
    qsem,
    main_ssem,
    main_rsem,
    ssem,
    rsem,
):
    z, x, c, y = place()
    band = lax.axis_index("band")
    sibling = (band + 1 - 2 * c, y)
    above, below = lax.rem(y + 1, 4), lax.rem(y + 3, 4)
    loads = [
        pltpu.make_async_copy(src, dst, load_sem.at[k])
        for k, (src, dst) in enumerate(
            (
                (grad_in, grad_ref),
                (slot_in, slot_ref),
                (latent_in, latent_ref),
                (mesh_in, patch.at[y]),
                (edge_in, edge_ref),
                (w_msg_in, w_msg_ref),
                (w_out_in, w_out_ref),
                (w_mesh_in, w_mesh_ref),
                (w_grid_in, w_grid_ref),
            )
        )
    ]
    for load in loads:
        load.start()
    bar = pltpu.get_barrier_semaphore()

    def greet(n, carry):
        to = band + n
        to = jnp.where(to < 32, to, to - 32)
        for k in range(4):
            pl.semaphore_signal(bar, inc=1, device_id=(to, k), device_id_type=MESH)
        return carry

    for k in (1, 2, 3):
        pl.semaphore_signal(
            bar, inc=1, device_id=(band, lax.rem(y + k, 4)), device_id_type=MESH
        )
    lax.fori_loop(1, 32, greet, 0)

    columns = [lax.rem(x + k, 4) * 2 for k in range(4)]
    cores = [c, 1 - c]
    cross = lax.rem(y + 2, 4)

    def bands(o, first=0):
        for i in range(first, 8):
            yield o * 8 + i, lax.rem(z + o + i, 4) * 8 + columns[i % 4] + cores[i // 4]

    def near(act):
        for v, to in bands(0, 1):
            act(v, (to, y))

        def run(o, carry):
            for v, to in bands(o):
                act(v, (to, y))
            return carry

        lax.fori_loop(1, 4, run, 0)

    def far(act):
        def beside(o, carry):
            for v, to in bands(o):
                act(32 + 2 * v, (to, above))
                act(33 + 2 * v, (to, below))
            return carry

        def opposite(o, carry):
            for v, to in bands(o):
                act(96 + v, (to, cross))
            return carry

        lax.fori_loop(0, 4, beside, 0)
        lax.fori_loop(0, 4, opposite, 0)

    loads[3].wait()
    pl.semaphore_wait(bar, NDEV - 1)
    half = pl.ds(0, 160)
    rest = pl.ds(160, 160)

    def patch_copy(n, block, to):
        return remote(block, block, psem.at[n], qsem.at[n], (band, to))

    up = patch_copy(0, patch.at[y, rest], above)
    down = patch_copy(1, patch.at[y, half], below)
    up_later = patch_copy(4, patch.at[y, half], above)
    down_later = patch_copy(5, patch.at[y, rest], below)
    up_half = patch_copy(2, patch.at[below, rest], above)
    down_half = patch_copy(3, patch.at[above, half], below)
    for copy in (up, down, up_later, down_later):
        copy.start()
    for k in (0, 1, 2):
        loads[k].wait()
    channels, points = grad_ref.shape
    me = band * 4 + y
    lane = lax.broadcasted_iota(jnp.int32, (1, points), 1)
    total = points * NDEV
    angle = jnp.pi * (((me * points + lane).astype(F32) + 0.5) / total - 0.5)
    weight = 0.5 * jnp.pi * jnp.cos(angle)
    weighted[...] = jnp.zeros_like(weighted)
    weighted[0:channels, :] = (weight * grad_ref[...].astype(F32)).astype(BF)
    slot = slot_ref[...].reshape(1, points)
    j = (slot * 3641) >> 16
    r = slot - j * CAP
    dy = (j - y) & 3
    i = (((j >> 3) - x) & 3) + 4 * (((j >> 2) - c) & 1)
    q = 8 * ((((j >> 5) - z) - i) & 3) + i
    d = jnp.where(dy == 0, q, jnp.where(dy == 2, 96 + q, 32 + 2 * q + (dy >> 1)))
    at_main = jnp.where(r < MAIN, d * MAIN + r, -1)
    at_over = jnp.where(r >= MAIN, d * OVER + r - MAIN, -1)
    row = lax.broadcasted_iota(jnp.int32, (ROWS, points), 0)

    def pick(at, base):
        hot = jnp.where(row == at - base, 1.0, 0.0).astype(BF)
        lat = dot(hot, latent_ref[...], NN).astype(BF)
        gr = dot(hot, weighted[...], NT).astype(BF)
        return lat, gr

    lat, gr = pick(at_over, 0)
    over_send[:, :, 0:512] = lat.reshape(NDEV, OVER, 512)
    over_send[:, :, 512:768] = gr.reshape(NDEV, OVER, 256)
    over_recv[0] = over_send[0]

    def pick_main(g):
        lat, gr = pick(at_main, g * ROWS)
        blocks = pl.ds(g * BLOCKS, BLOCKS)
        main_send[blocks, :, 0:512] = lat.reshape(BLOCKS, MAIN, 512)
        main_send[blocks, :, 512:768] = gr.reshape(BLOCKS, MAIN, 256)

    def send_over(d, device):
        remote(
            over_send.at[d], over_recv.at[d], ssem.at[1], rsem.at[1], device
        ).start()

    def send_main(d, device):
        remote(
            main_send.at[d],
            main_recv.at[d],
            main_ssem.at[0],
            main_rsem.at[lax.div(d, BLOCKS)],
            device,
        ).start()

    pick_main(0)
    pick_main(1)
    main_recv[0] = main_send[0]
    near(send_main)
    near(send_over)

    def prep_group(g, carry):
        pick_main(g)
        return carry

    lax.fori_loop(2, GROUPS - 1, prep_group, 0)
    up.wait_recv()
    up_half.start()
    down.wait_recv()
    down_half.start()
    far(send_over)
    far(send_main)
    for k in (4, 5, 6, 7, 8):
        loads[k].wait()
    back[...] = jnp.zeros_like(back)
    back[:, 0:channels] = dot(w_msg_ref[...], w_out_ref[...], NT).astype(BF)
    node[...] = jnp.zeros_like(node)
    outer_part[...] = jnp.zeros_like(outer_part)

    size = table.shape[0]
    local = edge_ref[...] - band * size
    halves = jnp.concatenate(
        [(local >> 4).astype(F32), (local & 15).astype(F32), jnp.zeros((2, SLOTS), F32)], axis=0
    ).astype(BF)
    lanes = lax.broadcasted_iota(jnp.int32, (ROWS, SLOTS), 1)
    line = lax.broadcasted_iota(jnp.int32, (ROWS, 1), 0)

    def find(g, slots):
        hot = jnp.where(lanes == slots, 1.0, 0.0).astype(BF)
        found = dot(halves, hot, NT)
        whole = (found[0:3] * 16.0 + found[3:6]).astype(jnp.int32)
        index_ref[g, 0:3, :] = whole

    def find_main(g, carry):
        find(g, source((g - 1) * BLOCKS + (line >> 4)) * CAP + (line & 15))
        return carry

    index_ref[...] = jnp.zeros_like(index_ref)
    find(0, source(line >> 1) * CAP + MAIN + (line & 1))
    lax.fori_loop(1, GROUPS, find_main, 0)

    up_half.wait_recv()
    down_half.wait_recv()
    up_later.wait_recv()
    down_later.wait_recv()
    for k in range(4):
        table[pl.ds(k * 320, 320), :] = dot(patch[k], w_mesh_ref[...], NN).astype(BF)

    def collect(g, carry):
        column = index_ref[g].T
        node_col = lax.broadcasted_iota(jnp.int32, (ROWS, size), 1)
        for k in range(3):
            hot = jnp.where(node_col == column[:, k : k + 1], 1.0, 0.0).astype(BF)
            gathered[g, k] = dot(hot, table[...], NN).astype(BF)
        return carry

    lax.fori_loop(0, GROUPS, collect, 0)
    patch_t[...] = patch[...].reshape(size, 512).T

    def group(g):
        latent, grad = rows_ref[:, 0:512], rows_ref[:, 512:768]
        grid_proj = dot(latent, w_grid_ref[...], NN).astype(BF).astype(F32)
        act_grad = dot(grad, back[...], NT)
        act = jnp.zeros((ROWS, 512), F32)
        total = jnp.zeros((ROWS, 512), F32)
        for k in range(3):
            pre = gathered[g, k].astype(F32) + grid_proj
            sigma = 0.5 * jnp.tanh(0.5 * pre) + 0.5
            value = pre * sigma
            act += value
            grad_k = (act_grad * (sigma + value * (1.0 - sigma))).astype(BF)
            total += grad_k.astype(F32)
            gathered[g, k] = grad_k
        act = act.astype(BF)
        moment = dot(act, grad, TN)
        across = dot(latent, total.astype(BF), TN)
        for h in range(2):
            outer_part[h, :, 0:256] += across[:, h * 256 : h * 256 + 256]
            outer_part[h, :, 256:384] += moment[:, h * 128 : h * 128 + 128]

    def spread(g):
        index = index_ref[g]
        node_row = lax.broadcasted_iota(jnp.int32, (size, ROWS), 0)
        hots = [
            jnp.where(node_row == index[k : k + 1, :], 1.0, 0.0).astype(BF)
            for k in range(3)
        ]
        values = gathered[g].reshape(3 * ROWS, 512)
        node[...] += dot(jnp.concatenate(hots, axis=1), values, NN)

    def await_main(g, first, count):
        blocks = pl.ds(first, count)
        remote(
            main_send.at[blocks], main_recv.at[blocks], main_ssem.at[0], main_rsem.at[g], sibling
        ).wait_recv()

    def load_main(g):
        blocks = pl.ds(g * BLOCKS, BLOCKS)
        rows_ref[...] = main_recv[blocks, :, :].reshape(ROWS, 768)

    def turn(i):
        return jnp.where(i < 2, i + 1, jnp.where(i == 2, 0, i))

    def step(i, carry):
        @pl.when(i > 0)
        def _():
            spread(turn(i - 1))

        @pl.when(i == 0)
        def _():
            await_main(0, 1, BLOCKS - 1)
            load_main(0)

        @pl.when(i == 1)
        def _():
            await_main(1, BLOCKS, BLOCKS)
            load_main(1)

        @pl.when(i == 2)
        def _():
            blocks = pl.ds(1, NDEV - 1)
            remote(
                over_send.at[blocks], over_recv.at[blocks], ssem.at[1], rsem.at[1], sibling
            ).wait_recv()
            rows_ref[...] = over_recv[...].reshape(ROWS, 768)

        @pl.when(i > 2)
        def _():
            await_main(i - 1, (i - 1) * BLOCKS, BLOCKS)
            load_main(i - 1)

        group(turn(i))
        return carry

    lax.fori_loop(0, GROUPS, step, 0)

    plane = z * 4 + x
    planes = []
    for k in range(1, 16):
        n = (5 * k) % 16
        to_z = lax.rem(z + n // 4, 4)
        planes.append(
            (k, (to_z * 8 + columns[n % 4] + c, y), to_z * 4 + lax.rem(x + n % 4, 4))
        )
    scale = 1.0 / math.sqrt(3.0 * points * NDEV)

    def chain(base, part, pair_recv, rs_send, rs_recv, ring, sums):
        width = part.shape[2]

        def lane(n):
            return ssem.at[base + n], rsem.at[base + n]

        pair = remote(part.at[1 - c], pair_recv, *lane(0), sibling)
        others = pl.ds(1, 15)
        scattered = remote(rs_send.at[others], rs_recv.at[others], *lane(1), sibling)
        three = ring.at[pl.ds(0, 3)]
        ringed = remote(three, three, *lane(2), sibling)
        most = sums.at[c, pl.ds(0, 15)]
        spread_out = remote(most, most, *lane(4), sibling)
        share = remote(sums.at[c], sums.at[c], *lane(5), sibling)

        def scatter():
            pair.wait_recv()
            rs_send[...] = (part[c] + pair_recv[...]).astype(BF).reshape(16, 32, width)

            for k, device, to in planes:
                remote(rs_send.at[to], rs_recv.at[k], *lane(1), device).start()
            rs_recv[0] = rs_send[plane]

        def circulate():
            scattered.wait_recv()
            whole = rs_recv[0].astype(F32)
            for k in range(1, 16):
                whole += rs_recv[k].astype(F32)
            ring[y] = whole.astype(BF)
            for k in (1, 2, 3):
                remote(
                    ring.at[y], ring.at[y], *lane(2), (band, lax.rem(y + k, 4))
                ).start()

        def gather():
            ringed.wait_recv()
            whole = ring[0].astype(F32)
            for k in range(1, 4):
                whole += ring[k].astype(F32)
            sums[c, plane] = (whole * scale).astype(BF)
            block = sums.at[c, plane]
            for _, device, _ in planes:
                remote(block, block, *lane(4), device).start()

        def swap():
            spread_out.wait_recv()
            share.start()

        def drain():
            for copy in (pair, scattered, ringed, spread_out):
                copy.wait_send()
            share.wait()

        return pair, scatter, circulate, gather, swap, drain

    a_pair, a_scatter, a_circulate, a_gather, a_swap, a_drain = chain(
        4, outer_part, outer_pair, outer_rs_send, outer_rs_recv, outer_ring, outer_ref
    )
    b_pair, b_scatter, b_circulate, b_gather, b_swap, b_drain = chain(
        10, inner_part, inner_pair, inner_rs_send, inner_rs_recv, inner_ring, inner_ref
    )

    def node_send_half(n, rows):
        for k in (1, 2, 3):
            to = lax.rem(y + k, 4)
            remote(
                node_send.at[to, rows], node_recv.at[k - 1, rows], ssem.at[n], rsem.at[n], (band, to)
            ).start()

    def node_wait(n, rows):
        return remote(
            node_send.at[pl.ds(0, 3), rows], node_recv.at[:, rows], ssem.at[n], rsem.at[n], sibling
        )

    a_pair.start()
    spread(GROUPS - 1)
    node_send[...] = node[...].astype(BF).reshape(4, 320, 512)
    across = dot(patch_t[...], node_send[...].reshape(size, 512), NN)
    for h in range(2):
        inner_part[h] = across[:, h * 256 : h * 256 + 256]
    b_pair.start()
    a_scatter()
    node_send_half(2, half)
    b_scatter()
    a_circulate()
    b_circulate()
    a_gather()
    b_gather()
    node_send_half(3, rest)
    a_swap()
    b_swap()
    first, second = node_wait(2, half), node_wait(3, rest)
    first.wait_recv()
    second.wait_recv()
    mine = node[pl.ds(y * 320, 320), :]
    proj_ref[...] = (
        mine + node_recv[0].astype(F32) + node_recv[1].astype(F32) + node_recv[2].astype(F32)
    ).astype(BF)

    for copy in (up, down, up_later, down_later, up_half, down_half, first, second):
        copy.wait_send()
    blocks = pl.ds(1, NDEV - 1)
    remote(over_send.at[blocks], over_recv.at[blocks], ssem.at[1], rsem.at[1], sibling).wait_send()
    remote(main_send.at[blocks], main_recv.at[blocks], main_ssem.at[0], main_rsem.at[0], sibling).wait_send()
    a_drain()
    b_drain()


def final_kernel(*refs):
    ins, outs, held, done, sems = refs[0:6], refs[6:11], refs[11:17], refs[17:22], refs[22]
    loads = [
        pltpu.make_async_copy(src, dst, sems.at[k])
        for k, (src, dst) in enumerate(zip(ins, held))
    ]
    for load in loads:
        load.start()
    stores = [
        pltpu.make_async_copy(src, dst, sems.at[6 + k])
        for k, (src, dst) in enumerate(zip(done, outs))
    ]
    outer_ref, inner_ref, proj_ref, w_mesh_ref, w_msg_ref, w_out_ref = held
    node_ref, mesh_ref, grid_ref, msg_ref, out_ref = done
    loads[1].wait()
    for h in range(2):
        mesh_ref[:, h * 256 : h * 256 + 256] = inner_ref[h].astype(F32).reshape(512, 256)
    stores[1].start()
    loads[0].wait()
    moment = []
    for h in range(2):
        whole = outer_ref[h].astype(F32).reshape(512, 384)
        grid_ref[:, h * 256 : h * 256 + 256] = whole[:, 0:256]
        moment.append(whole[:, 256:384])
    stores[2].start()
    moment = jnp.concatenate(moment, axis=1)[:, 0:227].astype(BF)
    loads[5].wait()
    msg_ref[...] = dot(moment, w_out_ref[...], NN)
    stores[3].start()
    loads[4].wait()
    out_ref[...] = dot(moment, w_msg_ref[...], TN)
    stores[4].start()
    loads[2].wait()
    loads[3].wait()
    node_ref[...] = dot(proj_ref[...], w_mesh_ref[...], NT).astype(BF)
    stores[0].start()
    for store in stores:
        store.wait()


def shards(grad_pred, grid_latent, mesh_latent, send_slot, edge_src, w_mesh, w_grid, w_msg, w_out):
    vmem = pltpu.VMEM
    w_out = w_out.T
    hbm = pl.BlockSpec(memory_space=pltpu.HBM)
    outer, inner, proj = pl.pallas_call(
        kernel,
        in_specs=[hbm] * 9,
        out_shape=[
            jax.ShapeDtypeStruct((2, 16, 32, 384), BF),
            jax.ShapeDtypeStruct((2, 16, 32, 256), BF),
            jax.ShapeDtypeStruct((320, 512), BF),
        ],
        scratch_shapes=[
            vmem((227, 768), BF),
            vmem((768, 512), BF),
            vmem((768,), jnp.int32),
            vmem((3, SLOTS), jnp.int32),
            vmem((512, 512), BF),
            vmem((512, 512), BF),
            vmem((512, 512), BF),
            vmem((227, 512), BF),
            pltpu.SemaphoreType.DMA((9,)),
            vmem((GROUPS, 8, ROWS), jnp.int32),
            vmem((GROUPS, 3, ROWS, 512), BF),
            vmem((256, 768), BF),
            vmem((NDEV, MAIN, 768), BF),
            vmem((NDEV, OVER, 768), BF),
            vmem((NDEV, MAIN, 768), BF),
            vmem((NDEV, OVER, 768), BF),
            vmem((4, 320, 512), BF),
            vmem((512, 1280), BF),
            vmem((1280, 512), BF),
            vmem((512, 256), BF),
            vmem((1280, 512), F32),
            vmem((4, 320, 512), BF),
            vmem((3, 320, 512), BF),
            vmem((ROWS, 768), BF),
            vmem((2, 512, 384), F32),
            vmem((512, 384), F32),
            vmem((16, 32, 384), BF),
            vmem((16, 32, 384), BF),
            vmem((4, 32, 384), BF),
            vmem((2, 512, 256), F32),
            vmem((512, 256), F32),
            vmem((16, 32, 256), BF),
            vmem((16, 32, 256), BF),
            vmem((4, 32, 256), BF),
            pltpu.SemaphoreType.DMA((6,)),
            pltpu.SemaphoreType.DMA((6,)),
            pltpu.SemaphoreType.DMA((1,)),
            pltpu.SemaphoreType.DMA((GROUPS - 1,)),
            pltpu.SemaphoreType.DMA((16,)),
            pltpu.SemaphoreType.DMA((16,)),
        ],
        compiler_params=pltpu.CompilerParams(
            collective_id=0, has_side_effects=True, vmem_limit_bytes=67_043_328
        ),
    )(grad_pred, grid_latent, mesh_latent, send_slot, edge_src, w_mesh, w_grid, w_msg, w_out)
    shapes = [
        ((320, 512), BF),
        ((512, 512), F32),
        ((512, 512), F32),
        ((512, 512), F32),
        ((227, 512), F32),
    ]
    operands = (outer, inner, proj, w_mesh, w_msg, w_out)
    *grads, out_grad = pl.pallas_call(
        final_kernel,
        out_shape=[jax.ShapeDtypeStruct(*shape) for shape in shapes],
        in_specs=[hbm] * 6,
        out_specs=[hbm] * 5,
        scratch_shapes=[
            *(vmem(operand.shape, BF) for operand in operands),
            *(vmem(*shape) for shape in shapes),
            pltpu.SemaphoreType.DMA((11,)),
        ],
        compiler_params=pltpu.CompilerParams(vmem_limit_bytes=67_043_328),
    )(*operands)
    return *grads, out_grad.T


def solution(mesh):
    both = ("band", "sub")
    placed = (P(None, both), P(both, None), P(both, None), P(both), P(None, both))
    return jax.shard_map(
        shards,
        mesh=mesh,
        in_specs=placed + (P(),) * 4,
        out_specs=(P(both, None), P(), P(), P(), P()),
        check_vma=False,
    )
```
